32 devices in a mesh: seq: 8 (over z, core), tp: 4 (over y, x).
Axes of the slice: x: 2, y: 2, z: 4, core: 2. Of those that a mesh axis runs over, the one named last changes fastest.
Arguments:
- hidden: bfloat16 [4096, 2048], P(('seq', 'tp')), may hold values from -5 to 5
- w_qkv: bfloat16 [2048, 3, 2048], P(None, None, 'tp'), may hold values from -0.125 to 0.125
- w_gate: bfloat16 [2048, 2048], P(None, 'tp'), may hold values from -0.125 to 0.125
- w_decay_beta: bfloat16 [2048, 2, 16], P(None, None, 'tp'), may hold values from -0.7 to 0.7
- conv_weight: bfloat16 [4, 3, 2048], P(None, None, 'tp'), may hold values from -2 to 2
- decay_rate: float32 [16], P('tp'), may hold values from 2e-05 to 0.05
- dt_bias: float32 [16], P('tp'), may hold values from -1 to 1
- norm_gain: float32 [128], replicated, may hold values from 0.1 to 1.9
Outputs:
- core: bfloat16 [4096, 2048], P('seq', 'tp')
The draws below stay inside these ranges and needn't reach their ends.
All inputs are finite; a program needn't handle non-finite values.
Results may differ from the reference program's by a relative error of at most 0.01.
Values may be sent and summed in bfloat16 or wider, within the bound.
A program may use at most 64 MiB of HBM per device.

```python
import math
import jax
import jax.numpy as jnp
from jax import lax

D = 2048
H = 16
DH = 128
KERNEL = 4
SEQ = 4096


def direction_signs(key):
    return jax.random.rademacher(jax.random.fold_in(key, 71), (D,), dtype=jnp.float32)


def slow_heads(key):
    order = jax.random.permutation(jax.random.fold_in(key, 72), H)
    count = 3 * H // 8
    return (order < count).astype(jnp.float32)


def draw_hidden(key, part):
    signs = direction_signs(key)
    noise_key = jax.random.fold_in(key, 73)
    noise = 0.9 * jax.random.truncated_normal(noise_key, -5.0, 5.0, (SEQ, D), jnp.float32)
    offset = 0.4
    return (noise + offset * signs[None, :]).astype(jnp.bfloat16)


def draw_w_decay_beta(key, part):
    signs = direction_signs(key)
    slow = slow_heads(key)
    base = jax.random.truncated_normal(jax.random.fold_in(key, 74), -5.0, 5.0, (D, 2, H), jnp.float32)
    base = base * (1.0 / math.sqrt(D))
    strength = jax.random.uniform(jax.random.fold_in(key, 75), (H,), jnp.float32, 10.0, 13.0)
    slow_column = -strength[None, :] * signs[:, None] * (1.0 / D) + 0.3 * base[:, 1, :]
    beta_column = slow[None, :] * slow_column + (1.0 - slow[None, :]) * base[:, 1, :]
    return jnp.stack([base[:, 0, :], beta_column], axis=1).astype(jnp.bfloat16)


def draw_decay_rate(key, part):
    slow = slow_heads(key)
    fraction = jax.random.uniform(jax.random.fold_in(key, 76), (H,), jnp.float32, 0.0, 1.0)
    slow_rate = jnp.exp(math.log(2e-05) + fraction * (math.log(0.00015) - math.log(2e-05)))
    fast_rate = jnp.exp(math.log(0.002) + fraction * (math.log(0.05) - math.log(0.002)))
    return jnp.where(slow > 0.5, slow_rate, fast_rate).astype(jnp.float32)


def levels(own_key, dims, shards, low, high):
    level = 1.0
    for axis_at, shards_of in shards:
        draws = jax.random.uniform(jax.random.fold_in(jax.random.fold_in(own_key, 6), axis_at), (shards_of,), jnp.float32, low / len(shards), high / len(shards))
        level = level * jnp.repeat(jnp.exp(draws), dims[axis_at] // shards_of).reshape((-1,) + (1,) * (len(dims) - 1 - axis_at))
    return level


def scatter_about(stream_key, extent, deviation, limit, shards=(), held_as=jnp.bfloat16):
    loudness = levels(stream_key, extent, shards, -0.22, 0.18) if shards else 1.0
    entries = jax.random.normal(stream_key, extent, jnp.float32) * deviation * loudness
    return jnp.minimum(jnp.maximum(entries, -limit), limit).astype(held_as)


def setup_inputs(seed: int = 0) -> dict:
    arg_keys = jax.random.split(jax.random.key(seed), 9)
    return {
        "hidden": draw_hidden(jax.random.fold_in(arg_keys[8], 71), 0),
        "w_qkv": scatter_about(arg_keys[1], (D, 3, H * DH), D ** -0.5, 0.125, ((2, 4),)),
        "w_gate": scatter_about(arg_keys[2], (D, H * DH), D ** -0.5, 0.125, ((1, 4),)),
        "w_decay_beta": draw_w_decay_beta(jax.random.fold_in(arg_keys[8], 71), 0),
        "conv_weight": scatter_about(arg_keys[4], (KERNEL, 3, H * DH), 0.5, 2.0, ((2, 4),)),
        "decay_rate": draw_decay_rate(jax.random.fold_in(arg_keys[8], 71), 0),
        "dt_bias": jnp.clip(jax.random.uniform(arg_keys[6], (H,), jnp.float32, -1.0, 1.0) * levels(arg_keys[6], (H,), ((0, 4),), -0.4, 0.0), -1.0, 1.0),
        "norm_gain": jnp.clip(1.0 + 0.18 * jax.random.normal(arg_keys[7], (DH,), jnp.float32), 0.1, 1.9),
    }


def unit_rows(matrix):
    return matrix * lax.rsqrt(lax.optimization_barrier(jnp.sum(matrix * matrix, axis=-1, keepdims=True)) + 1e-06)

def reference(hidden, w_qkv, w_gate, w_decay_beta, conv_weight, decay_rate, dt_bias, norm_gain):
    seq_total = hidden.shape[0]
    columns = H * DH
    projected = jnp.dot(hidden, w_qkv.reshape(D, 3 * columns), preferred_element_type=jnp.float32)
    projected = projected.astype(jnp.bfloat16).reshape(seq_total, 3, columns)
    padded = jnp.concatenate([jnp.zeros((KERNEL - 1, 3, columns), jnp.bfloat16), projected], axis=0)
    convolved = jnp.zeros((seq_total, 3, columns), jnp.float32)
    for offset in range(KERNEL):
        convolved = convolved + padded[offset:offset + seq_total].astype(jnp.float32) * conv_weight[offset].astype(jnp.float32)
    activated = jax.nn.silu(convolved).astype(jnp.bfloat16)
    scalars = jnp.dot(hidden, w_decay_beta.reshape(D, 2 * H), preferred_element_type=jnp.float32).reshape(seq_total, 2, H)
    log_decay = -decay_rate * jax.nn.softplus(scalars[:, 0] + dt_bias)
    write_rate = jax.nn.sigmoid(scalars[:, 1])
    branches = activated.astype(jnp.float32).reshape(seq_total, 3, H, DH)
    inv_root = 1.0 / math.sqrt(DH)
    queries = unit_rows(branches[:, 0]) * inv_root
    keys_in = unit_rows(branches[:, 1])
    values_in = branches[:, 2]

    def advance(state_history, inputs):
        single_query, single_key, value_row, decay_row, rate_row = inputs
        state_history = jnp.exp(decay_row)[:, None, None] * state_history
        retrieved_value = jnp.einsum('cd,cdn->cn', single_key, state_history, precision=lax.Precision.HIGHEST)
        state_history = state_history + rate_row[:, None, None] * single_key[:, :, None] * (value_row - retrieved_value)[:, None, :]
        return (state_history, jnp.einsum('cd,cdn->cn', single_query, state_history, precision=lax.Precision.HIGHEST))
    start_state = jnp.zeros((H, DH, DH), jnp.float32)
    _, state_output = lax.scan(advance, start_state, (queries, keys_in, values_in, log_decay, write_rate))
    gate_linear = jnp.dot(hidden, w_gate, preferred_element_type=jnp.float32).reshape(seq_total, H, DH)
    rms_scale = lax.rsqrt(lax.optimization_barrier(jnp.mean(state_output * state_output, axis=-1, keepdims=True)) + 1e-06)
    core = state_output * rms_scale * norm_gain * jax.nn.silu(gate_linear)
    return core.reshape(seq_total, columns).astype(jnp.bfloat16)
```

```python
import functools
import math

import jax
import jax.numpy as jnp
from jax import lax
from jax.experimental import pallas as pl
from jax.experimental.pallas import tpu as pltpu
from jax.sharding import PartitionSpec as P

MESH = pl.DeviceIdType.MESH
CHUNK = 128
RIM = 16
NT = (((1,), (1,)), ((), ()))
TN = (((0,), (0,)), ((), ()))


def low(value):
    return value.astype(jnp.bfloat16)


def dot(left, right, dims=(((1,), (0,)), ((), ()))):
    return lax.dot_general(low(left), low(right), dims, preferred_element_type=jnp.float32)


def peer_of(me, step, count):
    if count & (count - 1):
        return lax.rem(me + step, count)
    bit = 1
    while bit < count:
        if step & bit:
            me = me + bit - 2 * bit * lax.rem(me // bit, 2)
        bit *= 2
    return me


def silu(value):
    return value / (1.0 + jnp.exp(-value))


def unit_rows(matrix):
    return matrix * lax.rsqrt(jnp.sum(matrix * matrix, axis=-1, keepdims=True) + 1e-06)


def kernel(
    n_seq, n_tp, rate_hbm, bias_hbm, hidden, w_qkv, w_gate, wdb_hbm, conv_hbm, gain_hbm, out_ref,
    rate_ref, bias_ref, wdb_ref, conv_ref, gain_ref, small_sem,
    tokens, rim, weights, proj, state, outs, deltas, st_in, st_out,
    tok_send, tok_recv, w_sem, rim_send, rim_recv, st_send, st_recv,
    middle, mid_send, mid_recv, solves, q_runs, k_tails, attends, fades,
):
    seq, me = lax.axis_index("seq"), lax.axis_index("tp")
    rows = hidden.shape[0]
    total = tokens.shape[0]
    heads = rate_ref.shape[1]
    head_dim = gain_ref.shape[1]
    taps = conv_ref.shape[1]
    last_tp, last_seq = n_tp - 1, n_seq - 1
    square = n_tp == 4 and rows == CHUNK
    part = rows // 2

    own = pltpu.make_async_copy(hidden, tokens.at[pl.ds(me * rows, rows)], tok_recv.at[0, 0])
    own.start()
    loads = [pltpu.make_async_copy(w_qkv.at[b], weights.at[b], w_sem.at[b]) for b in range(3)]
    loads.append(pltpu.make_async_copy(w_gate, weights.at[3], w_sem.at[3]))
    small = [(rate_hbm, rate_ref), (bias_hbm, bias_ref), (wdb_hbm, wdb_ref), (conv_hbm, conv_ref), (gain_hbm, gain_ref)]
    smalls = [pltpu.make_async_copy(src, dst, small_sem.at[i]) for i, (src, dst) in enumerate(small)]
    for load in loads + smalls:
        load.start()

    barrier = pltpu.get_barrier_semaphore()

    def greet(where):
        pl.semaphore_signal(barrier, inc=1, device_id=where, device_id_type=MESH)

    for step in range(1, n_tp):
        greet({"tp": peer_of(me, step, n_tp)})

    @pl.when(seq > 0)
    def _():
        greet({"seq": seq - 1})

        @pl.when(me < last_tp)
        def _():
            greet({"seq": seq - 1, "tp": last_tp})

    @pl.when(seq < last_seq)
    def _():
        greet({"seq": seq + 1})

    before = (seq + last_seq) // n_seq
    after = (2 * last_seq - seq) // n_seq
    tail_owner = (me + 1) // n_tp
    pl.semaphore_wait(barrier, last_tp + before + after + after * tail_owner * last_tp)

    def token_copy(step):
        return pltpu.make_async_remote_copy(
            src_ref=hidden,
            dst_ref=tokens.at[pl.ds(me * rows, rows)],
            send_sem=tok_send.at[step, 0],
            recv_sem=tok_recv.at[step, 0],
            device_id={"tp": peer_of(me, step, n_tp)},
            device_id_type=MESH,
        )

    def part_copy(step, half):
        return pltpu.make_async_remote_copy(
            src_ref=hidden.at[pl.ds(half * part, part)],
            dst_ref=tokens.at[pl.ds(me * rows + half * part, part)],
            send_sem=tok_send.at[step, half],
            recv_sem=tok_recv.at[step, half],
            device_id={"tp": peer_of(me, step, n_tp)},
            device_id_type=MESH,
        )

    def relay_copy(half):
        there = tokens.at[pl.ds(peer_of(me, 2 - half, n_tp) * rows + half * part, part)]
        return pltpu.make_async_remote_copy(
            src_ref=there,
            dst_ref=there,
            send_sem=tok_send.at[3, half],
            recv_sem=tok_recv.at[3, half],
            device_id={"tp": peer_of(me, 1 + half, n_tp)},
            device_id_type=MESH,
        )

    def middle_copy(target):
        return pltpu.make_async_remote_copy(
            src_ref=hidden.at[pl.ds(rows - RIM, RIM)],
            dst_ref=middle,
            send_sem=mid_send.at[target - 2],
            recv_sem=mid_recv,
            device_id={"tp": target},
            device_id_type=MESH,
        )

    def rim_copy(target):
        return pltpu.make_async_remote_copy(
            src_ref=hidden.at[pl.ds(rows - RIM, RIM)],
            dst_ref=rim,
            send_sem=rim_send.at[target],
            recv_sem=rim_recv,
            device_id={"seq": seq + 1, "tp": target},
            device_id_type=MESH,
        )

    @pl.when(jnp.logical_and(seq < last_seq, me == last_tp))
    def _():
        for target in range(n_tp):
            rim_copy(target).start()

    if square:

        @pl.when(me == 1)
        def _():
            for target in (2, 3):
                middle_copy(target).start()

        for step, half in ((1, 1), (2, 0), (1, 0), (2, 1)):
            part_copy(step, half).start()
    else:
        for step in range(1, n_tp):
            token_copy(step).start()

    @pl.when(seq == 0)
    def _():
        rim[...] = jnp.zeros_like(rim)
        st_in[...] = jnp.zeros_like(st_in)

    for load in loads + smalls:
        load.wait()

    def project(block, at):
        def one(b, carry):
            full = jnp.dot(block, weights[b], preferred_element_type=jnp.float32)
            rounded = full.astype(jnp.bfloat16).astype(jnp.float32)
            proj[b, pl.ds(pl.multiple_of(at, 16), block.shape[0]), :] = jnp.where(b < 3, rounded, full)
            return carry

        lax.fori_loop(0, 4, one, 0)

    def project_slot(slot):
        at = pl.multiple_of(slot * rows, 16)
        project(tokens[pl.ds(at, rows), :], RIM + at)

    def project_rim():
        @pl.when(seq > 0)
        def _():
            pltpu.make_async_copy(hidden.at[pl.ds(0, RIM)], rim, rim_recv).wait()

        project(rim[...], 0)

    down = lax.broadcasted_iota(jnp.int32, (CHUNK, CHUNK), 0)
    across = lax.broadcasted_iota(jnp.int32, (CHUNK, CHUNK), 1)
    eye = (down == across).astype(jnp.float32)
    wide = lax.broadcasted_iota(jnp.int32, (head_dim, 2 * head_dim), 0) + head_dim
    start = (wide == lax.broadcasted_iota(jnp.int32, (head_dim, 2 * head_dim), 1)).astype(jnp.float32)
    for h in range(heads):
        state[h] = start

    wdb = low(jnp.concatenate([wdb_ref[0].astype(jnp.float32), wdb_ref[1].astype(jnp.float32)], axis=0))

    def prepare(c):
        r0 = pl.multiple_of(c * CHUNK, CHUNK)
        scalars = lax.dot_general(
            wdb, tokens[pl.ds(r0, CHUNK), :], NT, preferred_element_type=jnp.float32
        )
        per_head = []
        for h in range(heads):
            cols = slice(h * head_dim, (h + 1) * head_dim)
            branch = []
            for b in range(3):
                window = proj[b, pl.ds(r0 + 8, CHUNK + 8), cols]
                conv = jnp.zeros((CHUNK, head_dim), jnp.float32)
                for i in range(taps):
                    offset = 9 - taps + i
                    tap = conv_ref[b, i : i + 1, cols].astype(jnp.float32)
                    conv = conv + window[offset : offset + CHUNK] * tap
                branch.append(silu(conv).astype(jnp.bfloat16).astype(jnp.float32))
            q = unit_rows(branch[0]) * (1.0 / math.sqrt(head_dim))
            k = unit_rows(branch[1])
            v = branch[2]
            u = scalars[h : h + 1, :] + bias_ref[0:1, h : h + 1]
            log_row = -rate_ref[0:1, h : h + 1] * (jnp.maximum(u, 0.0) + jnp.log1p(jnp.exp(-jnp.abs(u))))
            rate_row = 1.0 / (1.0 + jnp.exp(-scalars[heads + h : heads + h + 1, :]))
            cum_col = jnp.sum(jnp.where(across <= down, log_row, 0.0), axis=1, keepdims=True)
            cum_row = jnp.sum(jnp.where(across == down, cum_col, 0.0), axis=0, keepdims=True)
            rate_col = jnp.sum(jnp.where(across == down, rate_row, 0.0), axis=1, keepdims=True)
            end = cum_col[CHUNK - 1 : CHUNK, :]
            gap = jnp.exp(jnp.where(across <= down, cum_col - cum_row, 0.0))
            weight = jnp.where(across <= down, gap, 0.0) * rate_row
            mixing = jnp.where(across < down, weight * dot(k, k, NT), 0.0)
            attend = weight * dot(q, k, NT)
            run = jnp.exp(cum_col)
            tail = rate_col * jnp.exp(end - cum_col)
            q_runs[c, h] = low(q * run)
            k_tails[c, h] = low(k * tail)
            attends[c, h] = low(attend)
            fades[c, h] = jnp.broadcast_to(jnp.exp(end), (1, head_dim))
            per_head.append((mixing, low(jnp.concatenate([v, k * run], axis=1))))
        return per_head

    def local(chunks):
        chains = [(c, h) + item for c in chunks for h, item in enumerate(prepare(c))]
        inverse = [None] * len(chains)
        size = 1
        while size < CHUNK:
            half = (down // size) % 2 == 1
            lower = jnp.logical_and(half, across // size == down // size - 1)
            for i, (_, _, mixing, _) in enumerate(chains):
                corner = jnp.where(lower, mixing, 0.0)
                if size == 1:
                    inverse[i] = eye - corner
                else:
                    inverse[i] = inverse[i] - dot(dot(inverse[i], corner), inverse[i])
            size *= 2
        for i, (c, h, _, right) in enumerate(chains):
            solves[c, h] = dot(inverse[i], right)

    def advance(c, carry):
        r0 = pl.multiple_of(c * CHUNK, CHUNK)
        for h in range(heads):
            solved = solves[c, h]
            held = state[h]
            fresh = solved[:, :head_dim]
            fresh = jnp.concatenate([fresh, jnp.zeros_like(fresh)], axis=1)
            fresh = fresh - dot(solved[:, head_dim:], held)
            read = dot(q_runs[c, h], held) + dot(attends[c, h], fresh)
            fade = jnp.concatenate([fades[c, h]] * 2, axis=1)
            state[h] = fade * held + dot(k_tails[c, h], fresh, TN)
            outs[h, pl.ds(r0, CHUNK), :] = read[:, :head_dim]
            deltas[h, pl.ds(r0, CHUNK), :] = low(read[:, head_dim:])
        return carry

    count = total // CHUNK
    own.wait()
    project_slot(me)
    if square:
        part_copy(1, 1).wait_recv()
        relay_copy(1).start()
        part_copy(2, 0).wait_recv()
        relay_copy(0).start()
        project_rim()

        @pl.when(me >= 2)
        def _():
            pltpu.make_async_copy(hidden.at[pl.ds(0, RIM)], middle, mid_recv).wait()
            project(middle[...], 2 * rows)

        part_copy(1, 0).wait_recv()
        project_slot(peer_of(me, 1, n_tp))
        first = 2 * (me // 2)
        local((first, first + 1))
        part_copy(2, 1).wait_recv()
        project_slot(peer_of(me, 2, n_tp))
        relay_copy(0).wait_recv()
        relay_copy(1).wait_recv()
        project_slot(peer_of(me, 3, n_tp))
        local((2 - first, 3 - first))
    else:
        for step in range(1, n_tp):
            token_copy(step).wait_recv()
            if n_tp & (n_tp - 1):
                project_slot(lax.rem(me - step + n_tp, n_tp))
            else:
                project_slot(peer_of(me, step, n_tp))
        project_rim()
        lax.fori_loop(0, count, lambda c, carry: (local((c,)), carry)[1], 0)
    lax.fori_loop(0, count, advance, 0, unroll=True)

    def state_copy(h):
        return pltpu.make_async_remote_copy(
            src_ref=st_out.at[h],
            dst_ref=st_in.at[h],
            send_sem=st_send.at[h],
            recv_sem=st_recv.at[h],
            device_id={"seq": seq + 1},
            device_id_type=MESH,
        )

    for h in range(heads):

        @pl.when(seq > 0)
        def _():
            pltpu.make_async_copy(st_out.at[h], st_in.at[h], st_recv.at[h]).wait()

        @pl.when(seq < last_seq)
        def _():
            mine = state[h]
            st_out[h] = low(mine[:, :head_dim] + dot(mine[:, head_dim:], st_in[h]))
            state_copy(h).start()

    for h in range(heads):
        cols = slice(h * head_dim, (h + 1) * head_dim)
        read = outs[h] + dot(deltas[h], st_in[h])
        scale = lax.rsqrt(jnp.mean(read * read, axis=-1, keepdims=True) + 1e-06)
        gate = silu(proj[3, pl.ds(RIM, total), cols])
        out_ref[:, cols] = low(read * scale * gain_ref[...] * gate)

    if square:
        for half in range(2):
            part_copy(1, half).wait_send()
            part_copy(2, half).wait_send()
            relay_copy(half).wait_send()

        @pl.when(me == 1)
        def _():
            for target in (2, 3):
                middle_copy(target).wait_send()
    else:
        for step in range(1, n_tp):
            token_copy(step).wait_send()

    @pl.when(jnp.logical_and(seq < last_seq, me == last_tp))
    def _():
        for target in range(n_tp):
            rim_copy(target).wait_send()

    @pl.when(seq < last_seq)
    def _():
        for h in range(heads):
            state_copy(h).wait_send()


def plain_device(
    n_seq, n_tp, hidden, w_qkv, w_gate, w_decay_beta, conv_weight, decay_rate, dt_bias, norm_gain
):
    width = hidden.shape[1]
    heads = decay_rate.shape[0]
    head_dim = norm_gain.shape[0]
    columns = heads * head_dim
    rows = hidden.shape[0]
    total = rows * n_tp
    vmem, anywhere = pl.BlockSpec(memory_space=pltpu.VMEM), pl.BlockSpec(memory_space=pl.ANY)
    dma = pltpu.SemaphoreType.DMA
    count = total // CHUNK
    return pl.pallas_call(
        functools.partial(kernel, n_seq, n_tp),
        out_shape=jax.ShapeDtypeStruct((total, columns), jnp.bfloat16),
        in_specs=[anywhere] * 8,
        out_specs=vmem,
        scratch_shapes=[
            pltpu.VMEM((1, heads), jnp.float32),
            pltpu.VMEM((1, heads), jnp.float32),
            pltpu.VMEM((2, heads, width), jnp.bfloat16),
            pltpu.VMEM((3, conv_weight.shape[0], columns), jnp.bfloat16),
            pltpu.VMEM((1, head_dim), jnp.float32),
            dma((5,)),
            pltpu.VMEM((total, width), jnp.bfloat16),
            pltpu.VMEM((RIM, width), jnp.bfloat16),
            pltpu.VMEM((4, width, columns), jnp.bfloat16),
            pltpu.VMEM((4, RIM + total, columns), jnp.float32),
            pltpu.VMEM((heads, head_dim, 2 * head_dim), jnp.float32),
            pltpu.VMEM((heads, total, head_dim), jnp.float32),
            pltpu.VMEM((heads, total, head_dim), jnp.bfloat16),
            pltpu.VMEM((heads, head_dim, head_dim), jnp.bfloat16),
            pltpu.VMEM((heads, head_dim, head_dim), jnp.bfloat16),
            dma((n_tp, 2)),
            dma((n_tp, 2)),
            dma((4,)),
            dma((n_tp,)),
            dma,
            dma((heads,)),
            dma((heads,)),
            pltpu.VMEM((RIM, width), jnp.bfloat16),
            dma((2,)),
            dma,
            pltpu.VMEM((count, heads, CHUNK, 2 * head_dim), jnp.float32),
            pltpu.VMEM((count, heads, CHUNK, head_dim), jnp.bfloat16),
            pltpu.VMEM((count, heads, CHUNK, head_dim), jnp.bfloat16),
            pltpu.VMEM((count, heads, CHUNK, CHUNK), jnp.bfloat16),
            pltpu.VMEM((count, heads, 1, head_dim), jnp.float32),
        ],
        compiler_params=pltpu.CompilerParams(
            collective_id=0, has_side_effects=True, vmem_limit_bytes=60 * 1024 * 1024
        ),
    )(
        decay_rate.reshape(1, heads), dt_bias.reshape(1, heads), hidden,
        w_qkv.transpose(1, 0, 2), w_gate, w_decay_beta.transpose(1, 2, 0),
        conv_weight.transpose(1, 0, 2), norm_gain.reshape(1, head_dim),
    )


def fast_kernel(
    n_seq, rate_hbm, bias_hbm, hidden, w_qkv, w_gate, wdb_hbm, conv_hbm, gain_hbm, out_ref,
    rate_ref, bias_ref, wdb_ref, conv_ref, gain_ref, small_sem,
    tokens, rim, weights, proj, gates, half_taps, masks,
    own_sem, tok_send, tok_recv, w_sem, rim_send, rim_recv,
    lows, rights, keys, tails, decays, runs, fades, solves, maps, prefixes, totals, qeffs, outs, deltas,
    map_out, map_in, fade_out, fade_in, joined, joined_b, joined_f,
    map_send, map_recv, fade_send, fade_recv,
    st_in, st_out, held, st_send, st_recv, fw_send,
):
    seq, me = lax.axis_index("seq"), lax.axis_index("tp")
    last_seq = n_seq - 1
    odd = lax.rem(seq, 2) == 1
    even = lax.rem(seq, 2) == 0
    rows = hidden.shape[0]
    total = tokens.shape[0]
    heads = rate_ref.shape[1]
    dim = gain_ref.shape[1]
    taps = conv_ref.shape[1]
    count = total // CHUNK
    split = 48
    tail_at = rows - RIM

    own = pltpu.make_async_copy(hidden, tokens.at[pl.ds(me * rows, rows)], own_sem)
    own.start()
    order = (1, 2, 0)
    loads = [pltpu.make_async_copy(w_qkv.at[b], weights.at[i], w_sem.at[i]) for i, b in enumerate(order)]
    loads.append(pltpu.make_async_copy(w_gate, weights.at[3], w_sem.at[3]))
    small = [(rate_hbm, rate_ref), (bias_hbm, bias_ref), (wdb_hbm, wdb_ref), (conv_hbm, conv_ref), (gain_hbm, gain_ref)]
    smalls = [pltpu.make_async_copy(src, dst, small_sem.at[i]) for i, (src, dst) in enumerate(small)]
    for load in loads + smalls:
        load.start()

    barrier = pltpu.get_barrier_semaphore()

    def greet(where):
        pl.semaphore_signal(barrier, inc=1, device_id=where, device_id_type=MESH)

    peers = [peer_of(me, step, 4) for step in range(4)]
    for step in range(1, 4):
        greet({"tp": peers[step]})

    @pl.when(seq > 0)
    def _():
        greet({"seq": seq - 1})

    @pl.when(seq < last_seq)
    def _():
        greet({"seq": seq + 1})

    @pl.when(jnp.logical_and(odd, seq > 1))
    def _():
        greet({"seq": seq - 2})

    @pl.when(jnp.logical_and(odd, seq < last_seq))
    def _():
        greet({"seq": seq + 2})

    is_odd = lax.rem(seq, 2)
    before = (seq + last_seq) // n_seq
    after = (2 * last_seq - seq) // n_seq
    before2 = (seq + n_seq - 2) // n_seq
    pl.semaphore_wait(barrier, 3 + before + after + is_odd * (before2 + after))

    pieces = ((0, split), (split, tail_at - split), (tail_at, RIM))

    def piece_copy(step, piece):
        at, size = pieces[piece]
        where = tokens.at[pl.ds(me * rows + at, size)]
        return pltpu.make_async_remote_copy(
            src_ref=where,
            dst_ref=where,
            send_sem=tok_send.at[step, piece],
            recv_sem=tok_recv.at[step, piece],
            device_id={"tp": peers[step]},
            device_id_type=MESH,
        )

    def relay_copy(half):
        at, size = pieces[half]
        there = tokens.at[pl.ds(peers[2 - half] * rows + at, size)]
        return pltpu.make_async_remote_copy(
            src_ref=there,
            dst_ref=there,
            send_sem=tok_send.at[3, half],
            recv_sem=tok_recv.at[3, half],
            device_id={"tp": peers[1 + half]},
            device_id_type=MESH,
        )

    def rim_copy():
        return pltpu.make_async_remote_copy(
            src_ref=tokens.at[pl.ds(total - RIM, RIM)],
            dst_ref=rim,
            send_sem=rim_send,
            recv_sem=rim_recv,
            device_id={"seq": seq + 1},
            device_id_type=MESH,
        )

    own.wait()
    for step in (3, 1, 2):
        piece_copy(step, 2).start()
    for step, half in ((1, 1), (2, 0), (1, 0), (2, 1)):
        piece_copy(step, half).start()

    @pl.when(seq == 0)
    def _():
        rim[...] = jnp.zeros_like(rim)

    down = lax.broadcasted_iota(jnp.int32, (CHUNK, CHUNK), 0)
    across = lax.broadcasted_iota(jnp.int32, (CHUNK, CHUNK), 1)
    eye = low((down == across).astype(jnp.float32))
    edges = (1, 2, 8, 32, CHUNK)
    for i in range(4):
        inside = down // edges[i + 1] == across // edges[i + 1]
        apart = down // edges[i] != across // edges[i]
        masks[i] = low(jnp.where(jnp.logical_and(inside, apart), 1.0, 0.0))

    for load in smalls:
        load.wait()
    for b in range(3):
        for i in range(taps):
            row = conv_ref[b, i : i + 1, :].astype(jnp.float32) * 0.5
            for h in range(heads):
                cols = slice(h * dim, (h + 1) * dim)
                half_taps[b, i, h] = jnp.broadcast_to(row[:, cols], (8, dim))
    wdb = low(jnp.concatenate([wdb_ref[0].astype(jnp.float32), wdb_ref[1].astype(jnp.float32)], axis=0))

    def project(block, slots, places):
        def one(b, carry):
            full = jnp.dot(block, weights[b], preferred_element_type=jnp.float32)
            full = full.astype(jnp.bfloat16).astype(jnp.float32)
            for start, size, at in places:
                for h in range(heads):
                    proj[b, h, pl.ds(at, size), :] = full[start : start + size, h * dim : (h + 1) * dim]
            return carry

        lax.fori_loop(slots[0], slots[1], one, 0)

    def project_gate(block, at):
        full = jnp.dot(block, weights[3], preferred_element_type=jnp.float32)
        for h in range(heads):
            gates[h, pl.ds(at, rows), :] = full[:, h * dim : (h + 1) * dim]

    def project_block(slot, slots, gate):
        at = pl.multiple_of(slot * rows, rows)
        block = tokens[pl.ds(at, rows), :]
        project(block, slots, ((0, rows, pl.multiple_of(at + RIM, RIM)),))
        if gate:
            project_gate(block, at)

    def half_silu(half):
        return half + half * jnp.tanh(half)

    def branch(b, h, r0):
        conv = None
        for i in range(taps):
            window = proj[b, h, pl.ds(r0 + (RIM + 1 - taps + i), CHUNK), :]
            term = window.reshape(CHUNK // 8, 8, dim) * half_taps[order[b], i, h][None]
            conv = term if conv is None else conv + term
        return half_silu(conv).astype(jnp.bfloat16).reshape(CHUNK, dim)

    def prepare(c):
        r0 = pl.multiple_of(c * CHUNK, CHUNK)
        scalars = lax.dot_general(
            wdb, tokens[pl.ds(r0, CHUNK), :], NT, preferred_element_type=jnp.float32
        )
        for h in range(heads):
            k = unit_rows(branch(0, h, r0).astype(jnp.float32))
            v = branch(1, h, r0)
            u = scalars[h : h + 1, :] + bias_ref[0:1, h : h + 1]
            log_row = -rate_ref[0:1, h : h + 1] * (jnp.maximum(u, 0.0) + jnp.log1p(jnp.exp(-jnp.abs(u))))
            rate_row = 1.0 / (1.0 + jnp.exp(-scalars[heads + h : heads + h + 1, :]))
            cum_col = jnp.sum(jnp.where(across <= down, log_row, 0.0), axis=1, keepdims=True)
            cum_row = jnp.sum(jnp.where(across == down, cum_col, 0.0), axis=0, keepdims=True)
            rate_col = jnp.sum(jnp.where(across == down, rate_row, 0.0), axis=1, keepdims=True)
            end = cum_col[CHUNK - 1 : CHUNK, :]
            gap = jnp.exp(jnp.where(across <= down, cum_col - cum_row, 0.0))
            weight = jnp.where(across <= down, gap, 0.0) * rate_row
            low_k = low(k)
            lows[c, h] = low(jnp.where(across < down, weight * dot(low_k, low_k, NT), 0.0))
            run = jnp.exp(cum_col)
            tail = rate_col * jnp.exp(end - cum_col)
            rights[c, h] = jnp.concatenate([v, low(k * run)], axis=1)
            tails[c, h] = low(k * tail)
            keys[c, h] = low_k
            decays[c, h] = weight
            runs[c, h] = jnp.broadcast_to(run, (CHUNK, dim))
            fades[c, h] = jnp.broadcast_to(jnp.exp(end), (1, dim))

    def solve(chunks):
        chains = [(c, h) for c in chunks for h in range(heads)]
        inverse = [eye - lows[c, h] * masks[0] for c, h in chains]
        for level in (1, 2):
            step = [low(dot(inverse[i], lows[c, h] * masks[level])) for i, (c, h) in enumerate(chains)]
            both = [dot(x, jnp.concatenate([low(d), x], axis=1)) for x, d in zip(step, inverse)]
            first = [d.astype(jnp.float32) - p[:, :CHUNK] for p, d in zip(both, inverse)]
            inverse = [q + dot(p[:, CHUNK:], q) for p, q in zip(both, first)]
        both = [
            dot(inverse[i], jnp.concatenate([lows[c, h] * masks[3], rights[c, h]], axis=1))
            for i, (c, h) in enumerate(chains)
        ]
        again = [dot(p[:, :CHUNK], p) for p in both]
        first = [p[:, CHUNK:] - a[:, CHUNK:] for p, a in zip(both, again)]
        for (c, h), a, q in zip(chains, again, first):
            solves[c, h] = low(q + dot(a[:, :CHUNK], q))
        for c, h in chains:
            got = dot(tails[c, h], solves[c, h], TN)
            maps[c, h] = jnp.concatenate([got[:, :dim], -got[:, dim:]], axis=1)

    def queries(c):
        r0 = pl.multiple_of(c * CHUNK, CHUNK)
        for h in range(heads):
            q = unit_rows(branch(2, h, r0).astype(jnp.float32)) * (1.0 / math.sqrt(dim))
            attend = decays[c, h] * dot(q, keys[c, h], NT)
            got = dot(attend, solves[c, h])
            outs[h, pl.ds(r0, CHUNK), :] = got[:, :dim]
            qeffs[h, pl.ds(r0, CHUNK), :] = q * runs[c, h] - got[:, dim:]

    loads[0].wait()
    loads[1].wait()
    project_block(me, (0, 2), False)
    loads[2].wait()
    loads[3].wait()
    project_block(me, (2, 3), True)

    for step in range(1, 4):
        piece_copy(step, 2).wait_recv()

    @pl.when(seq < last_seq)
    def _():
        rim_copy().start()

    @pl.when(seq > 0)
    def _():
        pltpu.make_async_copy(tokens.at[pl.ds(0, RIM)], rim, rim_recv).wait()

    places = [(0, RIM, 0)]
    edge_rows = [rim[...]]
    for step in range(1, 4):
        at = pl.multiple_of(peers[step] * rows + tail_at, RIM)
        edge_rows.append(tokens[pl.ds(at, RIM), :])
        places.append((step * RIM, RIM, pl.multiple_of(at + RIM, RIM)))
    project(jnp.concatenate(edge_rows, axis=0), (0, 3), places)

    prepare(me)
    piece_copy(1, 1).wait_recv()
    relay_copy(1).start()
    piece_copy(2, 0).wait_recv()
    relay_copy(0).start()
    solve((me,))
    queries(me)

    piece_copy(1, 0).wait_recv()
    project_block(peers[1], (0, 3), True)
    piece_copy(2, 1).wait_recv()
    project_block(peers[2], (0, 3), True)
    prepare(peers[1])
    prepare(peers[2])
    solve((peers[1], peers[2]))
    queries(peers[1])
    queries(peers[2])

    relay_copy(0).wait_recv()
    relay_copy(1).wait_recv()
    project_block(peers[3], (0, 2), False)
    prepare(peers[3])
    solve((peers[3],))

    def map_copy(h):
        return pltpu.make_async_remote_copy(
            src_ref=map_out.at[h], dst_ref=map_in.at[h], send_sem=map_send.at[h], recv_sem=map_recv.at[h],
            device_id={"seq": seq + 1}, device_id_type=MESH,
        )

    def fade_copy():
        return pltpu.make_async_remote_copy(
            src_ref=fade_out, dst_ref=fade_in, send_sem=fade_send, recv_sem=fade_recv,
            device_id={"seq": seq + 1}, device_id_type=MESH,
        )

    def state_copy(h):
        return pltpu.make_async_remote_copy(
            src_ref=st_out.at[h], dst_ref=st_in.at[h], send_sem=st_send.at[h], recv_sem=st_recv.at[h],
            device_id={"seq": seq + 2}, device_id_type=MESH,
        )

    def share_copy(h):
        return pltpu.make_async_remote_copy(
            src_ref=st_in.at[h], dst_ref=st_in.at[h], send_sem=fw_send.at[h], recv_sem=st_recv.at[h],
            device_id={"seq": seq - 1}, device_id_type=MESH,
        )

    for h in range(heads):
        whole = maps[0, h]
        fade = fades[0, h]
        for c in range(1, count):
            prefixes[c, h] = low(whole)
            totals[c, h] = fade
            mine, keep = maps[c, h], fades[c, h]
            got = dot(mine[:, dim:], whole)
            left = keep * whole[:, :dim] + mine[:, :dim] + got[:, :dim]
            right = keep * whole[:, dim:] + fade * mine[:, dim:] + got[:, dim:]
            whole = jnp.concatenate([left, right], axis=1)
            fade = keep * fade
        maps[0, h] = whole
        map_out[h] = low(whole)
        fade_out[h] = fade

    @pl.when(even)
    def _():
        fade_copy().start()
        for h in range(heads):
            map_copy(h).start()

    @pl.when(seq == 0)
    def _():
        for h in range(heads):
            held[h] = jnp.zeros((dim, dim), jnp.bfloat16)

    @pl.when(odd)
    def _():
        fade_copy().wait_recv()
        for h in range(heads):
            map_copy(h).wait_recv()
            whole, fade = maps[0, h], fade_out[h]
            other, its = map_in[h].astype(jnp.float32), fade_in[h]
            got = dot(whole[:, dim:], map_in[h])
            base = fade * other[:, :dim] + whole[:, :dim] + got[:, :dim]

            @pl.when(seq == 1)
            def _():
                held[h] = map_in[h, :, :dim]

                @pl.when(seq < last_seq)
                def _():
                    st_out[h] = low(base)
                    state_copy(h).start()

            joined_b[h] = base
            joined[h] = low(fade * other[:, dim:] + its * whole[:, dim:] + got[:, dim:])
            joined_f[h] = fade * its

    def pass_on():
        for h in range(heads):
            state_copy(h).wait_recv()
            share_copy(h).start()
            state = st_in[h]
            wide = state.astype(jnp.float32)

            @pl.when(seq < last_seq)
            def _():
                st_out[h] = low(joined_f[h] * wide + joined_b[h] + dot(joined[h], state))
                state_copy(h).start()

            other = map_in[h]
            held[h] = low(fade_in[h] * wide + other[:, :dim].astype(jnp.float32) + dot(other[:, dim:], state))

    @pl.when(jnp.logical_and(odd, seq == 3))
    def _():
        pass_on()

    project_block(peers[3], (2, 3), True)
    queries(peers[3])
    for c in range(count):
        at = pl.ds(c * CHUNK, CHUNK)
        for h in range(heads):
            qeff = qeffs[h, at, :]
            if c == 0:
                deltas[h, at, :] = low(qeff)
            else:
                got = dot(qeff, prefixes[c, h])
                outs[h, at, :] = outs[h, at, :] + got[:, :dim]
                deltas[h, at, :] = low(totals[c, h] * qeff + got[:, dim:])

    @pl.when(jnp.logical_and(odd, seq > 3))
    def _():
        pass_on()

    for h in range(heads):

        @pl.when(jnp.logical_and(even, seq > 0))
        def _():
            state_copy(h).wait_recv()
            held[h] = st_in[h]

        cols = slice(h * dim, (h + 1) * dim)
        read = outs[h] + dot(deltas[h], held[h])
        scale = lax.rsqrt(jnp.mean(read * read, axis=-1, keepdims=True) + 1e-06)
        out_ref[:, cols] = low(read * scale * gain_ref[...] * half_silu(0.5 * gates[h]))

    for step in range(1, 4):
        for piece in range(3):
            if step == 3 and piece < 2:
                relay_copy(piece).wait_send()
            else:
                piece_copy(step, piece).wait_send()

    @pl.when(seq < last_seq)
    def _():
        rim_copy().wait_send()

    @pl.when(even)
    def _():
        fade_copy().wait_send()
        for h in range(heads):
            map_copy(h).wait_send()

    @pl.when(jnp.logical_and(odd, seq > 1))
    def _():
        for h in range(heads):
            share_copy(h).wait_send()

    @pl.when(jnp.logical_and(odd, seq < last_seq))
    def _():
        for h in range(heads):
            state_copy(h).wait_send()


def fast_device(n_seq, hidden, w_qkv, w_gate, w_decay_beta, conv_weight, decay_rate, dt_bias, norm_gain):
    rows, width = hidden.shape
    heads = decay_rate.shape[0]
    dim = norm_gain.shape[0]
    taps = conv_weight.shape[0]
    columns = heads * dim
    total = rows * 4
    count = total // CHUNK
    dma = pltpu.SemaphoreType.DMA
    f32, bf16 = jnp.float32, jnp.bfloat16
    operands = (
        decay_rate.reshape(1, heads), dt_bias.reshape(1, heads), hidden,
        w_qkv.transpose(1, 0, 2), w_gate, w_decay_beta.transpose(1, 2, 0),
        conv_weight.transpose(1, 0, 2), norm_gain.reshape(1, dim),
    )
    return pl.pallas_call(
        functools.partial(fast_kernel, n_seq),
        out_shape=jax.ShapeDtypeStruct((total, columns), bf16),
        in_specs=[pl.BlockSpec(memory_space=pl.ANY)] * 8,
        out_specs=pl.BlockSpec(memory_space=pltpu.VMEM),
        scratch_shapes=[
            pltpu.VMEM((1, heads), f32),
            pltpu.VMEM((1, heads), f32),
            pltpu.VMEM((2, heads, width), bf16),
            pltpu.VMEM((3, taps, columns), bf16),
            pltpu.VMEM((1, dim), f32),
            dma((5,)),
            pltpu.VMEM((total, width), bf16),
            pltpu.VMEM((RIM, width), bf16),
            pltpu.VMEM((4, width, columns), bf16),
            pltpu.VMEM((3, heads, RIM + total, dim), f32),
            pltpu.VMEM((heads, total, dim), f32),
            pltpu.VMEM((3, taps, heads, 8, dim), f32),
            pltpu.VMEM((4, CHUNK, CHUNK), bf16),
            dma,
            dma((4, 3)),
            dma((4, 3)),
            dma((4,)),
            dma,
            dma,
            pltpu.VMEM((count, heads, CHUNK, CHUNK), bf16),
            pltpu.VMEM((count, heads, CHUNK, 2 * dim), bf16),
            pltpu.VMEM((count, heads, CHUNK, dim), bf16),
            pltpu.VMEM((count, heads, CHUNK, dim), bf16),
            pltpu.VMEM((count, heads, CHUNK, CHUNK), f32),
            pltpu.VMEM((count, heads, CHUNK, dim), f32),
            pltpu.VMEM((count, heads, 1, dim), f32),
            pltpu.VMEM((count, heads, CHUNK, 2 * dim), bf16),
            pltpu.VMEM((count, heads, dim, 2 * dim), f32),
            pltpu.VMEM((count, heads, dim, 2 * dim), bf16),
            pltpu.VMEM((count, heads, 1, dim), f32),
            pltpu.VMEM((heads, total, dim), f32),
            pltpu.VMEM((heads, total, dim), f32),
            pltpu.VMEM((heads, total, dim), bf16),
            pltpu.VMEM((heads, dim, 2 * dim), bf16),
            pltpu.VMEM((heads, dim, 2 * dim), bf16),
            pltpu.VMEM((heads, 1, dim), f32),
            pltpu.VMEM((heads, 1, dim), f32),
            pltpu.VMEM((heads, dim, dim), bf16),
            pltpu.VMEM((heads, dim, dim), f32),
            pltpu.VMEM((heads, 1, dim), f32),
            dma((heads,)),
            dma((heads,)),
            dma,
            dma,
            pltpu.VMEM((heads, dim, dim), bf16),
            pltpu.VMEM((heads, dim, dim), bf16),
            pltpu.VMEM((heads, dim, dim), bf16),
            dma((heads,)),
            dma((heads,)),
            dma((heads,)),
        ],
        compiler_params=pltpu.CompilerParams(
            collective_id=0, has_side_effects=True, vmem_limit_bytes=48 * 1024 * 1024
        ),
    )(*[pltpu.with_memory_space_constraint(x, pltpu.HBM) for x in operands])


def per_device(n_seq, n_tp, hidden, *rest):
    if n_tp == 4 and hidden.shape[0] == CHUNK and n_seq % 2 == 0:
        return fast_device(n_seq, hidden, *rest)
    return plain_device(n_seq, n_tp, hidden, *rest)


def solution(mesh):
    return jax.shard_map(
        functools.partial(per_device, mesh.shape["seq"], mesh.shape["tp"]),
        mesh=mesh,
        in_specs=(
            P(("seq", "tp"), None),
            P(None, None, "tp"),
            P(None, "tp"),
            P(None, None, "tp"),
            P(None, None, "tp"),
            P("tp"),
            P("tp"),
            P(),
        ),
        out_specs=P("seq", "tp"),
        check_vma=False,
    )
```

```python
import functools
import math

import jax
import jax.numpy as jnp
from jax import lax
from jax.experimental import pallas as pl
from jax.experimental.pallas import tpu as pltpu
from jax.sharding import PartitionSpec as P

MESH = pl.DeviceIdType.MESH
CHUNK = 128
RIM = 16
NT = (((1,), (1,)), ((), ()))
TN = (((0,), (0,)), ((), ()))


def low(value):
    return value.astype(jnp.bfloat16)


def dot(left, right, dims=(((1,), (0,)), ((), ()))):
    return lax.dot_general(low(left), low(right), dims, preferred_element_type=jnp.float32)


def peer_of(me, step, count):
    if count & (count - 1):
        return lax.rem(me + step, count)
    bit = 1
    while bit < count:
        if step & bit:
            me = me + bit - 2 * bit * lax.rem(me // bit, 2)
        bit *= 2
    return me


def silu(value):
    return value / (1.0 + jnp.exp(-value))


def unit_rows(matrix):
    return matrix * lax.rsqrt(jnp.sum(matrix * matrix, axis=-1, keepdims=True) + 1e-06)


def kernel(
    n_seq, n_tp, rate_hbm, bias_hbm, hidden, w_qkv, w_gate, wdb_hbm, conv_hbm, gain_hbm, out_ref,
    rate_ref, bias_ref, wdb_ref, conv_ref, gain_ref, small_sem,
    tokens, rim, weights, proj, state, outs, deltas, st_in, st_out,
    tok_send, tok_recv, w_sem, rim_send, rim_recv, st_send, st_recv,
    middle, mid_send, mid_recv, solves, q_runs, k_tails, attends, fades,
):
    seq, me = lax.axis_index("seq"), lax.axis_index("tp")
    rows = hidden.shape[0]
    total = tokens.shape[0]
    heads = rate_ref.shape[1]
    head_dim = gain_ref.shape[1]
    taps = conv_ref.shape[1]
    last_tp, last_seq = n_tp - 1, n_seq - 1
    square = n_tp == 4 and rows == CHUNK
    part = rows // 2

    own = pltpu.make_async_copy(hidden, tokens.at[pl.ds(me * rows, rows)], tok_recv.at[0, 0])
    own.start()
    loads = [pltpu.make_async_copy(w_qkv.at[b], weights.at[b], w_sem.at[b]) for b in range(3)]
    loads.append(pltpu.make_async_copy(w_gate, weights.at[3], w_sem.at[3]))
    small = [(rate_hbm, rate_ref), (bias_hbm, bias_ref), (wdb_hbm, wdb_ref), (conv_hbm, conv_ref), (gain_hbm, gain_ref)]
    smalls = [pltpu.make_async_copy(src, dst, small_sem.at[i]) for i, (src, dst) in enumerate(small)]
    for load in loads + smalls:
        load.start()

    barrier = pltpu.get_barrier_semaphore()

    def greet(where):
        pl.semaphore_signal(barrier, inc=1, device_id=where, device_id_type=MESH)

    for step in range(1, n_tp):
        greet({"tp": peer_of(me, step, n_tp)})

    @pl.when(seq > 0)
    def _():
        greet({"seq": seq - 1})

        @pl.when(me < last_tp)
        def _():
            greet({"seq": seq - 1, "tp": last_tp})

    @pl.when(seq < last_seq)
    def _():
        greet({"seq": seq + 1})

    before = (seq + last_seq) // n_seq
    after = (2 * last_seq - seq) // n_seq
    tail_owner = (me + 1) // n_tp
    pl.semaphore_wait(barrier, last_tp + before + after + after * tail_owner * last_tp)

    def token_copy(step):
        return pltpu.make_async_remote_copy(
            src_ref=hidden,
            dst_ref=tokens.at[pl.ds(me * rows, rows)],
            send_sem=tok_send.at[step, 0],
            recv_sem=tok_recv.at[step, 0],
            device_id={"tp": peer_of(me, step, n_tp)},
            device_id_type=MESH,
        )

    def part_copy(step, half):
        return pltpu.make_async_remote_copy(
            src_ref=hidden.at[pl.ds(half * part, part)],
            dst_ref=tokens.at[pl.ds(me * rows + half * part, part)],
            send_sem=tok_send.at[step, half],
            recv_sem=tok_recv.at[step, half],
            device_id={"tp": peer_of(me, step, n_tp)},
            device_id_type=MESH,
        )

    def relay_copy(half):
        there = tokens.at[pl.ds(peer_of(me, 2 - half, n_tp) * rows + half * part, part)]
        return pltpu.make_async_remote_copy(
            src_ref=there,
            dst_ref=there,
            send_sem=tok_send.at[3, half],
            recv_sem=tok_recv.at[3, half],
            device_id={"tp": peer_of(me, 1 + half, n_tp)},
            device_id_type=MESH,
        )

    def middle_copy(target):
        return pltpu.make_async_remote_copy(
            src_ref=hidden.at[pl.ds(rows - RIM, RIM)],
            dst_ref=middle,
            send_sem=mid_send.at[target - 2],
            recv_sem=mid_recv,
            device_id={"tp": target},
            device_id_type=MESH,
        )

    def rim_copy(target):
        return pltpu.make_async_remote_copy(
            src_ref=hidden.at[pl.ds(rows - RIM, RIM)],
            dst_ref=rim,
            send_sem=rim_send.at[target],
            recv_sem=rim_recv,
            device_id={"seq": seq + 1, "tp": target},
            device_id_type=MESH,
        )

    @pl.when(jnp.logical_and(seq < last_seq, me == last_tp))
    def _():
        for target in range(n_tp):
            rim_copy(target).start()

    if square:

        @pl.when(me == 1)
        def _():
            for target in (2, 3):
                middle_copy(target).start()

        for step, half in ((1, 1), (2, 0), (1, 0), (2, 1)):
            part_copy(step, half).start()
    else:
        for step in range(1, n_tp):
            token_copy(step).start()

    @pl.when(seq == 0)
    def _():
        rim[...] = jnp.zeros_like(rim)
        st_in[...] = jnp.zeros_like(st_in)

    for load in loads + smalls:
        load.wait()

    def project(block, at):
        def one(b, carry):
            full = jnp.dot(block, weights[b], preferred_element_type=jnp.float32)
            rounded = full.astype(jnp.bfloat16).astype(jnp.float32)
            proj[b, pl.ds(pl.multiple_of(at, 16), block.shape[0]), :] = jnp.where(b < 3, rounded, full)
            return carry

        lax.fori_loop(0, 4, one, 0)

    def project_slot(slot):
        at = pl.multiple_of(slot * rows, 16)
        project(tokens[pl.ds(at, rows), :], RIM + at)

    def project_rim():
        @pl.when(seq > 0)
        def _():
            pltpu.make_async_copy(hidden.at[pl.ds(0, RIM)], rim, rim_recv).wait()

        project(rim[...], 0)

    down = lax.broadcasted_iota(jnp.int32, (CHUNK, CHUNK), 0)
    across = lax.broadcasted_iota(jnp.int32, (CHUNK, CHUNK), 1)
    eye = (down == across).astype(jnp.float32)
    wide = lax.broadcasted_iota(jnp.int32, (head_dim, 2 * head_dim), 0) + head_dim
    start = (wide == lax.broadcasted_iota(jnp.int32, (head_dim, 2 * head_dim), 1)).astype(jnp.float32)
    for h in range(heads):
        state[h] = start

    wdb = low(jnp.concatenate([wdb_ref[0].astype(jnp.float32), wdb_ref[1].astype(jnp.float32)], axis=0))

    def prepare(c):
        r0 = pl.multiple_of(c * CHUNK, CHUNK)
        scalars = lax.dot_general(
            wdb, tokens[pl.ds(r0, CHUNK), :], NT, preferred_element_type=jnp.float32
        )
        per_head = []
        for h in range(heads):
            cols = slice(h * head_dim, (h + 1) * head_dim)
            branch = []
            for b in range(3):
                window = proj[b, pl.ds(r0 + 8, CHUNK + 8), cols]
                conv = jnp.zeros((CHUNK, head_dim), jnp.float32)
                for i in range(taps):
                    offset = 9 - taps + i
                    tap = conv_ref[b, i : i + 1, cols].astype(jnp.float32)
                    conv = conv + window[offset : offset + CHUNK] * tap
                branch.append(silu(conv).astype(jnp.bfloat16).astype(jnp.float32))
            q = unit_rows(branch[0]) * (1.0 / math.sqrt(head_dim))
            k = unit_rows(branch[1])
            v = branch[2]
            u = scalars[h : h + 1, :] + bias_ref[0:1, h : h + 1]
            log_row = -rate_ref[0:1, h : h + 1] * (jnp.maximum(u, 0.0) + jnp.log1p(jnp.exp(-jnp.abs(u))))
            rate_row = 1.0 / (1.0 + jnp.exp(-scalars[heads + h : heads + h + 1, :]))
            cum_col = jnp.sum(jnp.where(across <= down, log_row, 0.0), axis=1, keepdims=True)
            cum_row = jnp.sum(jnp.where(across == down, cum_col, 0.0), axis=0, keepdims=True)
            rate_col = jnp.sum(jnp.where(across == down, rate_row, 0.0), axis=1, keepdims=True)
            end = cum_col[CHUNK - 1 : CHUNK, :]
            gap = jnp.exp(jnp.where(across <= down, cum_col - cum_row, 0.0))
            weight = jnp.where(across <= down, gap, 0.0) * rate_row
            mixing = jnp.where(across < down, weight * dot(k, k, NT), 0.0)
            attend = weight * dot(q, k, NT)
            run = jnp.exp(cum_col)
            tail = rate_col * jnp.exp(end - cum_col)
            q_runs[c, h] = low(q * run)
            k_tails[c, h] = low(k * tail)
            attends[c, h] = low(attend)
            fades[c, h] = jnp.broadcast_to(jnp.exp(end), (1, head_dim))
            per_head.append((mixing, low(jnp.concatenate([v, k * run], axis=1))))
        return per_head

    def local(chunks):
        chains = [(c, h) + item for c in chunks for h, item in enumerate(prepare(c))]
        inverse = [None] * len(chains)
        size = 1
        while size < CHUNK:
            half = (down // size) % 2 == 1
            lower = jnp.logical_and(half, across // size == down // size - 1)
            for i, (_, _, mixing, _) in enumerate(chains):
                corner = jnp.where(lower, mixing, 0.0)
                if size == 1:
                    inverse[i] = eye - corner
                else:
                    inverse[i] = inverse[i] - dot(dot(inverse[i], corner), inverse[i])
            size *= 2
        for i, (c, h, _, right) in enumerate(chains):
            solves[c, h] = dot(inverse[i], right)

    def advance(c, carry):
        r0 = pl.multiple_of(c * CHUNK, CHUNK)
        for h in range(heads):
            solved = solves[c, h]
            held = state[h]
            fresh = solved[:, :head_dim]
            fresh = jnp.concatenate([fresh, jnp.zeros_like(fresh)], axis=1)
            fresh = fresh - dot(solved[:, head_dim:], held)
            read = dot(q_runs[c, h], held) + dot(attends[c, h], fresh)
            fade = jnp.concatenate([fades[c, h]] * 2, axis=1)
            state[h] = fade * held + dot(k_tails[c, h], fresh, TN)
            outs[h, pl.ds(r0, CHUNK), :] = read[:, :head_dim]
            deltas[h, pl.ds(r0, CHUNK), :] = low(read[:, head_dim:])
        return carry

    count = total // CHUNK
    own.wait()
    project_slot(me)
    if square:
        part_copy(1, 1).wait_recv()
        relay_copy(1).start()
        part_copy(2, 0).wait_recv()
        relay_copy(0).start()
        project_rim()

        @pl.when(me >= 2)
        def _():
            pltpu.make_async_copy(hidden.at[pl.ds(0, RIM)], middle, mid_recv).wait()
            project(middle[...], 2 * rows)

        part_copy(1, 0).wait_recv()
        project_slot(peer_of(me, 1, n_tp))
        first = 2 * (me // 2)
        local((first, first + 1))
        part_copy(2, 1).wait_recv()
        project_slot(peer_of(me, 2, n_tp))
        relay_copy(0).wait_recv()
        relay_copy(1).wait_recv()
        project_slot(peer_of(me, 3, n_tp))
        local((2 - first, 3 - first))
    else:
        for step in range(1, n_tp):
            token_copy(step).wait_recv()
            if n_tp & (n_tp - 1):
                project_slot(lax.rem(me - step + n_tp, n_tp))
            else:
                project_slot(peer_of(me, step, n_tp))
        project_rim()
        lax.fori_loop(0, count, lambda c, carry: (local((c,)), carry)[1], 0)
    lax.fori_loop(0, count, advance, 0, unroll=True)

    def state_copy(h):
        return pltpu.make_async_remote_copy(
            src_ref=st_out.at[h],
            dst_ref=st_in.at[h],
            send_sem=st_send.at[h],
            recv_sem=st_recv.at[h],
            device_id={"seq": seq + 1},
            device_id_type=MESH,
        )

    for h in range(heads):

        @pl.when(seq > 0)
        def _():
            pltpu.make_async_copy(st_out.at[h], st_in.at[h], st_recv.at[h]).wait()

        @pl.when(seq < last_seq)
        def _():
            mine = state[h]
            st_out[h] = low(mine[:, :head_dim] + dot(mine[:, head_dim:], st_in[h]))
            state_copy(h).start()

    for h in range(heads):
        cols = slice(h * head_dim, (h + 1) * head_dim)
        read = outs[h] + dot(deltas[h], st_in[h])
        scale = lax.rsqrt(jnp.mean(read * read, axis=-1, keepdims=True) + 1e-06)
        gate = silu(proj[3, pl.ds(RIM, total), cols])
        out_ref[:, cols] = low(read * scale * gain_ref[...] * gate)

    if square:
        for half in range(2):
            part_copy(1, half).wait_send()
            part_copy(2, half).wait_send()
            relay_copy(half).wait_send()

        @pl.when(me == 1)
        def _():
            for target in (2, 3):
                middle_copy(target).wait_send()
    else:
        for step in range(1, n_tp):
            token_copy(step).wait_send()

    @pl.when(jnp.logical_and(seq < last_seq, me == last_tp))
    def _():
        for target in range(n_tp):
            rim_copy(target).wait_send()

    @pl.when(seq < last_seq)
    def _():
        for h in range(heads):
            state_copy(h).wait_send()


def plain_device(
    n_seq, n_tp, hidden, w_qkv, w_gate, w_decay_beta, conv_weight, decay_rate, dt_bias, norm_gain
):
    width = hidden.shape[1]
    heads = decay_rate.shape[0]
    head_dim = norm_gain.shape[0]
    columns = heads * head_dim
    rows = hidden.shape[0]
    total = rows * n_tp
    vmem, anywhere = pl.BlockSpec(memory_space=pltpu.VMEM), pl.BlockSpec(memory_space=pl.ANY)
    dma = pltpu.SemaphoreType.DMA
    count = total // CHUNK
    return pl.pallas_call(
        functools.partial(kernel, n_seq, n_tp),
        out_shape=jax.ShapeDtypeStruct((total, columns), jnp.bfloat16),
        in_specs=[anywhere] * 8,
        out_specs=vmem,
        scratch_shapes=[
            pltpu.VMEM((1, heads), jnp.float32),
            pltpu.VMEM((1, heads), jnp.float32),
            pltpu.VMEM((2, heads, width), jnp.bfloat16),
            pltpu.VMEM((3, conv_weight.shape[0], columns), jnp.bfloat16),
            pltpu.VMEM((1, head_dim), jnp.float32),
            dma((5,)),
            pltpu.VMEM((total, width), jnp.bfloat16),
            pltpu.VMEM((RIM, width), jnp.bfloat16),
            pltpu.VMEM((4, width, columns), jnp.bfloat16),
            pltpu.VMEM((4, RIM + total, columns), jnp.float32),
            pltpu.VMEM((heads, head_dim, 2 * head_dim), jnp.float32),
            pltpu.VMEM((heads, total, head_dim), jnp.float32),
            pltpu.VMEM((heads, total, head_dim), jnp.bfloat16),
            pltpu.VMEM((heads, head_dim, head_dim), jnp.bfloat16),
            pltpu.VMEM((heads, head_dim, head_dim), jnp.bfloat16),
            dma((n_tp, 2)),
            dma((n_tp, 2)),
            dma((4,)),
            dma((n_tp,)),
            dma,
            dma((heads,)),
            dma((heads,)),
            pltpu.VMEM((RIM, width), jnp.bfloat16),
            dma((2,)),
            dma,
            pltpu.VMEM((count, heads, CHUNK, 2 * head_dim), jnp.float32),
            pltpu.VMEM((count, heads, CHUNK, head_dim), jnp.bfloat16),
            pltpu.VMEM((count, heads, CHUNK, head_dim), jnp.bfloat16),
            pltpu.VMEM((count, heads, CHUNK, CHUNK), jnp.bfloat16),
            pltpu.VMEM((count, heads, 1, head_dim), jnp.float32),
        ],
        compiler_params=pltpu.CompilerParams(
            collective_id=0, has_side_effects=True, vmem_limit_bytes=60 * 1024 * 1024
        ),
    )(
        decay_rate.reshape(1, heads), dt_bias.reshape(1, heads), hidden,
        w_qkv.transpose(1, 0, 2), w_gate, w_decay_beta.transpose(1, 2, 0),
        conv_weight.transpose(1, 0, 2), norm_gain.reshape(1, head_dim),
    )


def fast_kernel(
    n_seq, rate_hbm, bias_hbm, hidden, w_qkv, w_gate, wdb_hbm, conv_hbm, gain_hbm, out_ref,
    rate_ref, bias_ref, wdb_ref, conv_ref, gain_ref, small_sem,
    tokens, rim, weights, proj_k, proj_v, proj_q, gates, half_taps, masks,
    own_sem, tok_send, tok_recv, w_sem, rim_send, rim_recv,
    betas, keys, decays, runs, fades, solves, maps, pairs, pair_fades, qeffs, outs, deltas,
    map_out, map_in, fade_out, fade_in, joined, joined_b, joined_f, far_in, far_fade,
    map_send, map_recv, fade_send, fade_recv, far_send, far_recv, far_fade_send, far_fade_recv,
    st_in, st_out, held, st_send, st_recv, fw_send, skip_send,
):
    seq, me = lax.axis_index("seq"), lax.axis_index("tp")
    last_seq = n_seq - 1
    odd = lax.rem(seq, 2) == 1
    even = lax.rem(seq, 2) == 0
    rows = hidden.shape[0]
    total = tokens.shape[0]
    heads = rate_ref.shape[1]
    dim = gain_ref.shape[1]
    taps = conv_ref.shape[1]
    count = total // CHUNK
    half_rows = rows // 2
    proj = (proj_k, proj_v, proj_q)
    tail_at = rows - RIM

    own = pltpu.make_async_copy(hidden, tokens.at[pl.ds(me * rows, rows)], own_sem)
    own.start()
    order = (1, 2, 0)
    loads = [pltpu.make_async_copy(w_qkv.at[b], weights.at[i], w_sem.at[i]) for i, b in enumerate(order)]
    loads.append(pltpu.make_async_copy(w_gate, weights.at[3], w_sem.at[3]))
    small = [(rate_hbm, rate_ref), (bias_hbm, bias_ref), (wdb_hbm, wdb_ref), (conv_hbm, conv_ref), (gain_hbm, gain_ref)]
    smalls = [pltpu.make_async_copy(src, dst, small_sem.at[i]) for i, (src, dst) in enumerate(small)]
    for load in smalls:
        load.start()

    barrier = pltpu.get_barrier_semaphore()

    def greet(where):
        pl.semaphore_signal(barrier, inc=1, device_id=where, device_id_type=MESH)

    peers = [peer_of(me, step, 4) for step in range(4)]
    for step in range(1, 3):
        greet({"tp": peers[step]})

    @pl.when(seq > 0)
    def _():
        greet({"seq": seq - 1})

    @pl.when(seq < last_seq)
    def _():
        greet({"seq": seq + 1})

    @pl.when(jnp.logical_and(odd, seq > 1))
    def _():
        greet({"seq": seq - 2})

    @pl.when(jnp.logical_and(odd, seq < last_seq))
    def _():
        greet({"seq": seq + 2})

    @pl.when(seq == last_seq)
    def _():
        greet({"seq": last_seq - 4})

    @pl.when(seq == last_seq - 4)
    def _():
        greet({"seq": last_seq})

    is_odd = lax.rem(seq, 2)
    before = (seq + last_seq) // n_seq
    after = (2 * last_seq - seq) // n_seq
    before2 = (seq + n_seq - 2) // n_seq
    skips = seq // last_seq + ((seq + 1) // (last_seq - 3)) * ((last_seq - 3) // (seq + 1))
    pl.semaphore_wait(barrier, 2 + before + after + is_odd * (before2 + after) + skips)

    quarter = half_rows // 2
    pieces = ((0, quarter), (quarter, quarter), (half_rows, tail_at - half_rows), (tail_at, RIM))

    def piece_copy(step, piece):
        at, size = pieces[piece]
        where = tokens.at[pl.ds(me * rows + at, size)]
        return pltpu.make_async_remote_copy(
            src_ref=where,
            dst_ref=where,
            send_sem=tok_send.at[step, piece],
            recv_sem=tok_recv.at[step, piece],
            device_id={"tp": peers[step]},
            device_id_type=MESH,
        )

    def relay_copy(piece):
        at, size = pieces[piece]
        via = 1 if piece < 2 else 2
        there = tokens.at[pl.ds(peers[3 - via] * rows + at, size)]
        return pltpu.make_async_remote_copy(
            src_ref=there,
            dst_ref=there,
            send_sem=tok_send.at[3, piece],
            recv_sem=tok_recv.at[3, piece],
            device_id={"tp": peers[via]},
            device_id_type=MESH,
        )

    def rim_copy():
        return pltpu.make_async_remote_copy(
            src_ref=tokens.at[pl.ds(total - RIM, RIM)],
            dst_ref=rim,
            send_sem=rim_send,
            recv_sem=rim_recv,
            device_id={"seq": seq + 1},
            device_id_type=MESH,
        )

    own.wait()
    for step, piece in ((1, 3), (2, 3), (1, 2), (2, 0)):
        piece_copy(step, piece).start()
    for load in loads:
        load.start()

    @pl.when(seq == 0)
    def _():
        rim[...] = jnp.zeros_like(rim)

    down = lax.broadcasted_iota(jnp.int32, (CHUNK, CHUNK), 0)
    across = lax.broadcasted_iota(jnp.int32, (CHUNK, CHUNK), 1)
    eye = low((down == across).astype(jnp.float32))
    edges = (1, 2, 8, 32, CHUNK)
    for i in range(4):
        inside = down // edges[i + 1] == across // edges[i + 1]
        apart = down // edges[i] != across // edges[i]
        masks[i] = low(jnp.where(jnp.logical_and(inside, apart), 1.0, 0.0))

    for load in smalls:
        load.wait()
    for b in range(3):
        for i in range(taps):
            row = conv_ref[b, i : i + 1, :].astype(jnp.float32) * 0.5
            for h in range(heads):
                cols = slice(h * dim, (h + 1) * dim)
                half_taps[b, i, h] = jnp.broadcast_to(row[:, cols], (8, dim))
    wdb = low(jnp.concatenate([wdb_ref[0].astype(jnp.float32), wdb_ref[1].astype(jnp.float32)], axis=0))

    def project(block, branches, places):
        for b in branches:
            full = jnp.dot(block, weights[b], preferred_element_type=jnp.float32)
            if b < 3:
                full = full.astype(jnp.bfloat16).astype(jnp.float32)
            for start, size, at, edge in places:
                for h in range(heads):
                    got = full[start : start + size, h * dim : (h + 1) * dim]
                    if b < 3:
                        proj[b][h, pl.ds(pl.multiple_of(at + RIM, RIM), size), :] = got
                    elif not edge:
                        gates[h, pl.ds(pl.multiple_of(at, RIM), size), :] = got

    def take(runs_of_rows):
        blocks, places, start = [], [], 0
        for slot, at, size in runs_of_rows:
            begin = pl.multiple_of(slot * rows + at, RIM)
            blocks.append(tokens[pl.ds(begin, size), :])
            places.append((start, size, begin, size == RIM))
            start += size
        return jnp.concatenate(blocks, axis=0), places

    def half_silu(half):
        return half + half * jnp.tanh(half)

    def branch(b, h, r0):
        conv = None
        for i in range(taps):
            window = proj[b][h, pl.ds(r0 + (RIM + 1 - taps + i), CHUNK), :]
            term = window.reshape(CHUNK // 8, 8, dim) * half_taps[order[b], i, h][None]
            conv = term if conv is None else conv + term
        return half_silu(conv).astype(jnp.bfloat16).reshape(CHUNK, dim)

    def gate_rows(c):
        r0 = pl.multiple_of(c * CHUNK, CHUNK)
        scalars = lax.dot_general(
            wdb, tokens[pl.ds(r0, CHUNK), :], NT, preferred_element_type=jnp.float32
        )
        for h in range(heads):
            u = scalars[h : h + 1, :] + bias_ref[0:1, h : h + 1]
            log_row = -rate_ref[0:1, h : h + 1] * (jnp.maximum(u, 0.0) + jnp.log1p(jnp.exp(-jnp.abs(u))))
            rate_row = 1.0 / (1.0 + jnp.exp(-scalars[heads + h : heads + h + 1, :]))
            cum_col = jnp.sum(jnp.where(across <= down, log_row, 0.0), axis=1, keepdims=True)
            cum_row = jnp.sum(jnp.where(across == down, cum_col, 0.0), axis=0, keepdims=True)
            rate_col = jnp.sum(jnp.where(across == down, rate_row, 0.0), axis=1, keepdims=True)
            end = cum_col[CHUNK - 1 : CHUNK, :]
            gap = jnp.exp(jnp.where(across <= down, cum_col - cum_row, 0.0))
            decays[c, h] = jnp.where(across <= down, gap, 0.0) * rate_row
            runs[c, h] = jnp.broadcast_to(jnp.exp(cum_col), (CHUNK, dim))
            betas[c, h] = jnp.broadcast_to(rate_col * jnp.exp(end - cum_col), (CHUNK, dim))
            fades[c, h] = jnp.broadcast_to(jnp.exp(end), (1, dim))

    def prepare(c):
        r0 = pl.multiple_of(c * CHUNK, CHUNK)
        chains = []
        for h in range(heads):
            k = unit_rows(branch(0, h, r0).astype(jnp.float32))
            low_k = low(k)
            keys[c, h] = low_k
            mixing = low(jnp.where(across < down, decays[c, h] * dot(low_k, low_k, NT), 0.0))
            chains.append((c, h, mixing, low(k * runs[c, h]), low(k * betas[c, h]), branch(1, h, r0)))
        return chains

    def solve(chains):
        inverse = [eye - mixing * masks[0] for _, _, mixing, _, _, _ in chains]
        for level in (1, 2):
            step = [low(dot(d, item[2] * masks[level])) for d, item in zip(inverse, chains)]
            both = [dot(x, jnp.concatenate([low(d), x], axis=1)) for x, d in zip(step, inverse)]
            first = [d.astype(jnp.float32) - p[:, :CHUNK] for p, d in zip(both, inverse)]
            inverse = [q + dot(p[:, CHUNK:], q) for p, q in zip(both, first)]
        both = [
            dot(d, jnp.concatenate([mixing * masks[3], v, k_run], axis=1))
            for d, (_, _, mixing, k_run, _, v) in zip(inverse, chains)
        ]
        again = [dot(p[:, :CHUNK], p) for p in both]
        first = [p[:, CHUNK:] - a[:, CHUNK:] for p, a in zip(both, again)]
        solved = [low(q + dot(a[:, :CHUNK], q)) for a, q in zip(again, first)]
        for item, value in zip(chains, solved):
            c, h = item[:2]
            solves[c, h] = value
            got = dot(item[4], value, TN)
            maps[c, h] = jnp.concatenate([got[:, :dim], -got[:, dim:]], axis=1)

    def queries(c):
        r0 = pl.multiple_of(c * CHUNK, CHUNK)
        for h in range(heads):
            q = unit_rows(branch(2, h, r0).astype(jnp.float32)) * (1.0 / math.sqrt(dim))
            attend = decays[c, h] * dot(q, keys[c, h], NT)
            got = dot(attend, solves[c, h])
            outs[h, pl.ds(r0, CHUNK), :] = got[:, :dim]
            qeffs[h, pl.ds(r0, CHUNK), :] = q * runs[c, h] - got[:, dim:]

    def join(late, early):
        (high, keep), (whole, fade) = late, early
        got = dot(high[:, dim:], whole)
        left = keep * whole[:, :dim] + high[:, :dim] + got[:, :dim]
        right = keep * whole[:, dim:] + fade * high[:, dim:] + got[:, dim:]
        return jnp.concatenate([left, right], axis=1), keep * fade

    def pair_up(p):
        for h in range(heads):
            whole, fade = join((maps[2 * p + 1, h], fades[2 * p + 1, h]), (maps[2 * p, h], fades[2 * p, h]))
            pairs[p, h] = whole
            pair_fades[p, h] = fade

    piece_copy(1, 3).wait_recv()
    relay_copy(3).start()
    for step, piece in ((1, 0), (1, 1), (2, 1), (2, 2)):
        piece_copy(step, piece).start()

    for load in loads:
        load.wait()
    block, places = take(((me, 0, rows),))
    project(block, range(4), places)

    piece_copy(2, 3).wait_recv()
    relay_copy(3).wait_recv()

    @pl.when(seq < last_seq)
    def _():
        rim_copy().start()

    piece_copy(1, 2).wait_recv()
    relay_copy(2).start()
    piece_copy(2, 0).wait_recv()
    relay_copy(0).start()

    @pl.when(seq > 0)
    def _():
        pltpu.make_async_copy(tokens.at[pl.ds(0, RIM)], rim, rim_recv).wait()

    block, places = take(((peers[1], half_rows, half_rows), (peers[2], 0, quarter), (peers[3], tail_at, RIM)))
    block = jnp.concatenate([block, rim[...]], axis=0)
    project(block, range(4), places + [(rows - RIM, RIM, -RIM, True)])
    piece_copy(2, 1).wait_recv()
    relay_copy(1).start()
    gate_rows(me)
    solve(prepare(me))
    queries(me)

    piece_copy(1, 0).wait_recv()
    piece_copy(1, 1).wait_recv()
    piece_copy(2, 2).wait_recv()
    late, late_places = take(((peers[1], 0, half_rows), (peers[2], quarter, rows - quarter)))
    gate_rows(peers[1])
    gate_rows(peers[2])
    project(late, range(2), late_places)
    solve(prepare(peers[1]) + prepare(peers[2]))
    pair_up(me // 2)

    for piece in range(3):
        relay_copy(piece).wait_recv()
    block, places = take(((peers[3], 0, rows),))
    gate_rows(peers[3])
    project(block, range(2), places)
    solve(prepare(peers[3]))
    pair_up(1 - me // 2)

    def map_copy(h):
        return pltpu.make_async_remote_copy(
            src_ref=map_out.at[h], dst_ref=map_in.at[h], send_sem=map_send.at[h], recv_sem=map_recv.at[h],
            device_id={"seq": seq + 1}, device_id_type=MESH,
        )

    def fade_copy():
        return pltpu.make_async_remote_copy(
            src_ref=fade_out, dst_ref=fade_in, send_sem=fade_send, recv_sem=fade_recv,
            device_id={"seq": seq + 1}, device_id_type=MESH,
        )

    def state_copy(h):
        return pltpu.make_async_remote_copy(
            src_ref=st_out.at[h], dst_ref=st_in.at[h], send_sem=st_send.at[h], recv_sem=st_recv.at[h],
            device_id={"seq": seq + 2}, device_id_type=MESH,
        )

    def skip_copy(h):
        return pltpu.make_async_remote_copy(
            src_ref=st_out.at[h], dst_ref=st_in.at[h], send_sem=skip_send.at[h], recv_sem=st_recv.at[h],
            device_id={"seq": seq + 4}, device_id_type=MESH,
        )

    def far_copy(h):
        return pltpu.make_async_remote_copy(
            src_ref=map_out.at[h], dst_ref=far_in.at[h], send_sem=far_send.at[h], recv_sem=far_recv.at[h],
            device_id={"seq": seq + 2}, device_id_type=MESH,
        )

    def far_fade_copy():
        return pltpu.make_async_remote_copy(
            src_ref=joined_f, dst_ref=far_fade, send_sem=far_fade_send, recv_sem=far_fade_recv,
            device_id={"seq": seq + 2}, device_id_type=MESH,
        )

    def share_copy(h, source):
        return pltpu.make_async_remote_copy(
            src_ref=source.at[h], dst_ref=st_in.at[h], send_sem=fw_send.at[h], recv_sem=st_recv.at[h],
            device_id={"seq": seq - 1}, device_id_type=MESH,
        )

    @pl.when(even)
    def _():
        for h in range(heads):
            whole, fade = join((pairs[1, h], pair_fades[1, h]), (pairs[0, h], pair_fades[0, h]))
            map_out[h] = low(whole)
            fade_out[h] = fade
            map_copy(h).start()
        fade_copy().start()

    @pl.when(seq == 0)
    def _():
        for h in range(heads):
            held[h] = jnp.zeros((dim, dim), jnp.bfloat16)

    def send_on(skip):
        def send(h):
            if skip:
                skip_copy(h).start()
            else:
                state_copy(h).start()

        return send

    def whole_map(h):
        return join((pairs[1, h], pair_fades[1, h]), (pairs[0, h], pair_fades[0, h]))

    def sent_map(h):
        return map_in[h].astype(jnp.float32), fade_in[h]

    def begin(skip):
        mine = [whole_map(h) for h in range(heads)]
        fade_copy().wait_recv()
        for h in range(heads):
            map_copy(h).wait_recv()
            (whole, fade), state = mine[h], map_in[h, :, :dim]
            base = fade * state.astype(jnp.float32) + whole[:, :dim]
            st_out[h] = low(base + dot(whole[:, dim:], state))
            send_on(skip)(h)
        for h in range(heads):
            held[h] = map_in[h, :, :dim]
            if skip:
                state_copy(h).start()

    def compose():
        mine = [whole_map(h) for h in range(heads)]
        fade_copy().wait_recv()
        for h in range(heads):
            map_copy(h).wait_recv()
        both = [join(mine[h], sent_map(h)) for h in range(heads)]
        for h, (whole, fade) in enumerate(both):
            joined_b[h] = whole[:, :dim]
            joined[h] = whole[:, dim:]
            joined_f[h] = fade
            map_out[h] = low(whole)

        @pl.when(seq == last_seq - 2)
        def _():
            for h in range(heads):
                far_copy(h).start()
            far_fade_copy().start()

    @pl.when(seq == 1)
    def _():
        begin(last_seq == 5)

    @pl.when(jnp.logical_and(jnp.logical_and(odd, seq > 1), seq < last_seq))
    def _():
        compose()

    def carry(h, state, whole, fade):
        wide = state.astype(jnp.float32)
        return low(fade * wide + whole[:, :dim].astype(jnp.float32) + dot(whole[:, dim:], state))

    def pass_on(more, skip):
        for h in range(heads):
            state_copy(h).wait_recv()
            if more:
                state = st_in[h]
                wide = joined_f[h] * state.astype(jnp.float32) + joined_b[h]
                st_out[h] = low(wide + dot(joined[h], state))
                send_on(skip)(h)
            share_copy(h, st_in).start()
        for h in range(heads):
            if more and skip:
                state_copy(h).start()
            held[h] = carry(h, st_in[h], map_in[h], fade_in[h])

    def end_chain():
        fade_copy().wait_recv()
        far_fade_copy().wait_recv()
        for h in range(heads):
            map_copy(h).wait_recv()
            far_copy(h).wait_recv()
        for h in range(heads):
            whole, fade = join(sent_map(h), (far_in[h].astype(jnp.float32), far_fade[h]))
            joined_b[h] = whole[:, :dim]
            joined[h] = whole[:, dim:]
            joined_f[h] = fade
        for h in range(heads):
            state_copy(h).wait_recv()
            state = st_in[h]
            st_out[h] = carry(h, state, far_in[h], far_fade[h])
            share_copy(h, st_out).start()
            wide = joined_f[h] * state.astype(jnp.float32) + joined_b[h]
            held[h] = low(wide + dot(joined[h], state))

    project(late, range(2, 4), late_places)
    queries(peers[1])
    queries(peers[2])

    @pl.when(jnp.logical_and(jnp.logical_and(odd, seq > 1), seq < last_seq - 4))
    def _():
        pass_on(True, False)

    if last_seq > 5:

        @pl.when(seq == last_seq - 4)
        def _():
            pass_on(True, True)

    project(block, range(2, 4), places)
    queries(peers[3])
    for h in range(heads):
        third, fade = join((maps[2, h], fades[2, h]), (pairs[0, h], pair_fades[0, h]))
        for c in range(count):
            at = pl.ds(c * CHUNK, CHUNK)
            qeff = qeffs[h, at, :]
            if c == 0:
                deltas[h, at, :] = low(qeff)
            else:
                prefix, keep = (
                    (maps[0, h], fades[0, h]), (pairs[0, h], pair_fades[0, h]), (third, fade)
                )[c - 1]
                got = dot(qeff, prefix)
                outs[h, at, :] = outs[h, at, :] + got[:, :dim]
                deltas[h, at, :] = low(keep * qeff + got[:, dim:])

    @pl.when(seq == last_seq - 2)
    def _():
        pass_on(False, False)

    @pl.when(seq == last_seq)
    def _():
        end_chain()

    for h in range(heads):

        @pl.when(jnp.logical_and(even, seq > 0))
        def _():
            state_copy(h).wait_recv()
            held[h] = st_in[h]

        cols = slice(h * dim, (h + 1) * dim)
        read = outs[h] + dot(deltas[h], held[h])
        scale = lax.rsqrt(jnp.mean(read * read, axis=-1, keepdims=True) + 1e-06)
        out_ref[:, cols] = low(read * scale * gain_ref[...] * half_silu(0.5 * gates[h]))

    for step in range(1, 4):
        for piece in range(4):
            if step == 3:
                relay_copy(piece).wait_send()
            else:
                piece_copy(step, piece).wait_send()

    @pl.when(seq < last_seq)
    def _():
        rim_copy().wait_send()

    @pl.when(even)
    def _():
        fade_copy().wait_send()
        for h in range(heads):
            map_copy(h).wait_send()

    @pl.when(jnp.logical_and(odd, seq > 1))
    def _():
        for h in range(heads):
            share_copy(h, st_in).wait_send()

    @pl.when(jnp.logical_and(odd, seq <= last_seq - 4))
    def _():
        for h in range(heads):
            state_copy(h).wait_send()

    @pl.when(seq == last_seq - 4)
    def _():
        for h in range(heads):
            skip_copy(h).wait_send()

    @pl.when(seq == last_seq - 2)
    def _():
        far_fade_copy().wait_send()
        for h in range(heads):
            far_copy(h).wait_send()


def fast_device(n_seq, hidden, w_qkv, w_gate, w_decay_beta, conv_weight, decay_rate, dt_bias, norm_gain):
    rows, width = hidden.shape
    heads = decay_rate.shape[0]
    dim = norm_gain.shape[0]
    taps = conv_weight.shape[0]
    columns = heads * dim
    total = rows * 4
    count = total // CHUNK
    dma = pltpu.SemaphoreType.DMA
    f32, bf16 = jnp.float32, jnp.bfloat16
    operands = (
        decay_rate.reshape(1, heads), dt_bias.reshape(1, heads), hidden,
        w_qkv.transpose(1, 0, 2), w_gate, w_decay_beta.transpose(1, 2, 0),
        conv_weight.transpose(1, 0, 2), norm_gain.reshape(1, dim),
    )
    return pl.pallas_call(
        functools.partial(fast_kernel, n_seq),
        out_shape=jax.ShapeDtypeStruct((total, columns), bf16),
        in_specs=[pl.BlockSpec(memory_space=pl.ANY)] * 8,
        out_specs=pl.BlockSpec(memory_space=pltpu.VMEM),
        scratch_shapes=[
            pltpu.VMEM((1, heads), f32),
            pltpu.VMEM((1, heads), f32),
            pltpu.VMEM((2, heads, width), bf16),
            pltpu.VMEM((3, taps, columns), bf16),
            pltpu.VMEM((1, dim), f32),
            dma((5,)),
            pltpu.VMEM((total, width), bf16),
            pltpu.VMEM((RIM, width), bf16),
            pltpu.VMEM((4, width, columns), bf16),
            pltpu.VMEM((heads, RIM + total, dim), f32),
            pltpu.VMEM((heads, RIM + total, dim), f32),
            pltpu.VMEM((heads, RIM + total, dim), f32),
            pltpu.VMEM((heads, total, dim), f32),
            pltpu.VMEM((3, taps, heads, 8, dim), f32),
            pltpu.VMEM((4, CHUNK, CHUNK), bf16),
            dma,
            dma((4, 4)),
            dma((4, 4)),
            dma((4,)),
            dma,
            dma,
            pltpu.VMEM((count, heads, CHUNK, dim), f32),
            pltpu.VMEM((count, heads, CHUNK, dim), bf16),
            pltpu.VMEM((count, heads, CHUNK, CHUNK), f32),
            pltpu.VMEM((count, heads, CHUNK, dim), f32),
            pltpu.VMEM((count, heads, 1, dim), f32),
            pltpu.VMEM((count, heads, CHUNK, 2 * dim), bf16),
            pltpu.VMEM((count, heads, dim, 2 * dim), f32),
            pltpu.VMEM((2, heads, dim, 2 * dim), f32),
            pltpu.VMEM((2, heads, 1, dim), f32),
            pltpu.VMEM((heads, total, dim), f32),
            pltpu.VMEM((heads, total, dim), f32),
            pltpu.VMEM((heads, total, dim), bf16),
            pltpu.VMEM((heads, dim, 2 * dim), bf16),
            pltpu.VMEM((heads, dim, 2 * dim), bf16),
            pltpu.VMEM((heads, 1, dim), f32),
            pltpu.VMEM((heads, 1, dim), f32),
            pltpu.VMEM((heads, dim, dim), f32),
            pltpu.VMEM((heads, dim, dim), f32),
            pltpu.VMEM((heads, 1, dim), f32),
            pltpu.VMEM((heads, dim, 2 * dim), bf16),
            pltpu.VMEM((heads, 1, dim), f32),
            dma((heads,)),
            dma((heads,)),
            dma,
            dma,
            dma((heads,)),
            dma((heads,)),
            dma,
            dma,
            pltpu.VMEM((heads, dim, dim), bf16),
            pltpu.VMEM((heads, dim, dim), bf16),
            pltpu.VMEM((heads, dim, dim), bf16),
            dma((heads,)),
            dma((heads,)),
            dma((heads,)),
            dma((heads,)),
        ],
        compiler_params=pltpu.CompilerParams(
            collective_id=0, has_side_effects=True, vmem_limit_bytes=48 * 1024 * 1024
        ),
    )(*[pltpu.with_memory_space_constraint(x, pltpu.HBM) for x in operands])


def per_device(n_seq, n_tp, hidden, *rest):
    if n_tp == 4 and hidden.shape[0] == CHUNK and n_seq % 2 == 0 and n_seq >= 6:
        return fast_device(n_seq, hidden, *rest)
    return plain_device(n_seq, n_tp, hidden, *rest)


def solution(mesh):
    return jax.shard_map(
        functools.partial(per_device, mesh.shape["seq"], mesh.shape["tp"]),
        mesh=mesh,
        in_specs=(
            P(("seq", "tp"), None),
            P(None, None, "tp"),
            P(None, "tp"),
            P(None, None, "tp"),
            P(None, None, "tp"),
            P("tp"),
            P("tp"),
            P(),
        ),
        out_specs=P("seq", "tp"),
        check_vma=False,
    )
```

```python
import functools
import math

import jax
import jax.numpy as jnp
from jax import lax
from jax.experimental import pallas as pl
from jax.experimental.pallas import tpu as pltpu
from jax.sharding import PartitionSpec as P

MESH = pl.DeviceIdType.MESH
CHUNK = 128
RIM = 16
NT = (((1,), (1,)), ((), ()))
TN = (((0,), (0,)), ((), ()))


def low(value):
    return value.astype(jnp.bfloat16)


def dot(left, right, dims=(((1,), (0,)), ((), ()))):
    return lax.dot_general(low(left), low(right), dims, preferred_element_type=jnp.float32)


def peer_of(me, step, count):
    if count & (count - 1):
        return lax.rem(me + step, count)
    bit = 1
    while bit < count:
        if step & bit:
            me = me + bit - 2 * bit * lax.rem(me // bit, 2)
        bit *= 2
    return me


def silu(value):
    return value / (1.0 + jnp.exp(-value))


def unit_rows(matrix):
    return matrix * lax.rsqrt(jnp.sum(matrix * matrix, axis=-1, keepdims=True) + 1e-06)


def kernel(
    n_seq, n_tp, rate_hbm, bias_hbm, hidden, w_qkv, w_gate, wdb_hbm, conv_hbm, gain_hbm, out_ref,
    rate_ref, bias_ref, wdb_ref, conv_ref, gain_ref, small_sem,
    tokens, rim, weights, proj, state, outs, deltas, st_in, st_out,
    tok_send, tok_recv, w_sem, rim_send, rim_recv, st_send, st_recv,
    middle, mid_send, mid_recv, solves, q_runs, k_tails, attends, fades,
):
    seq, me = lax.axis_index("seq"), lax.axis_index("tp")
    rows = hidden.shape[0]
    total = tokens.shape[0]
    heads = rate_ref.shape[1]
    head_dim = gain_ref.shape[1]
    taps = conv_ref.shape[1]
    last_tp, last_seq = n_tp - 1, n_seq - 1
    square = n_tp == 4 and rows == CHUNK
    part = rows // 2

    own = pltpu.make_async_copy(hidden, tokens.at[pl.ds(me * rows, rows)], tok_recv.at[0, 0])
    own.start()
    loads = [pltpu.make_async_copy(w_qkv.at[b], weights.at[b], w_sem.at[b]) for b in range(3)]
    loads.append(pltpu.make_async_copy(w_gate, weights.at[3], w_sem.at[3]))
    small = [(rate_hbm, rate_ref), (bias_hbm, bias_ref), (wdb_hbm, wdb_ref), (conv_hbm, conv_ref), (gain_hbm, gain_ref)]
    smalls = [pltpu.make_async_copy(src, dst, small_sem.at[i]) for i, (src, dst) in enumerate(small)]
    for load in loads + smalls:
        load.start()

    barrier = pltpu.get_barrier_semaphore()

    def greet(where):
        pl.semaphore_signal(barrier, inc=1, device_id=where, device_id_type=MESH)

    for step in range(1, n_tp):
        greet({"tp": peer_of(me, step, n_tp)})

    @pl.when(seq > 0)
    def _():
        greet({"seq": seq - 1})

        @pl.when(me < last_tp)
        def _():
            greet({"seq": seq - 1, "tp": last_tp})

    @pl.when(seq < last_seq)
    def _():
        greet({"seq": seq + 1})

    before = (seq + last_seq) // n_seq
    after = (2 * last_seq - seq) // n_seq
    tail_owner = (me + 1) // n_tp
    pl.semaphore_wait(barrier, last_tp + before + after + after * tail_owner * last_tp)

    def token_copy(step):
        return pltpu.make_async_remote_copy(
            src_ref=hidden,
            dst_ref=tokens.at[pl.ds(me * rows, rows)],
            send_sem=tok_send.at[step, 0],
            recv_sem=tok_recv.at[step, 0],
            device_id={"tp": peer_of(me, step, n_tp)},
            device_id_type=MESH,
        )

    def part_copy(step, half):
        return pltpu.make_async_remote_copy(
            src_ref=hidden.at[pl.ds(half * part, part)],
            dst_ref=tokens.at[pl.ds(me * rows + half * part, part)],
            send_sem=tok_send.at[step, half],
            recv_sem=tok_recv.at[step, half],
            device_id={"tp": peer_of(me, step, n_tp)},
            device_id_type=MESH,
        )

    def relay_copy(half):
        there = tokens.at[pl.ds(peer_of(me, 2 - half, n_tp) * rows + half * part, part)]
        return pltpu.make_async_remote_copy(
            src_ref=there,
            dst_ref=there,
            send_sem=tok_send.at[3, half],
            recv_sem=tok_recv.at[3, half],
            device_id={"tp": peer_of(me, 1 + half, n_tp)},
            device_id_type=MESH,
        )

    def middle_copy(target):
        return pltpu.make_async_remote_copy(
            src_ref=hidden.at[pl.ds(rows - RIM, RIM)],
            dst_ref=middle,
            send_sem=mid_send.at[target - 2],
            recv_sem=mid_recv,
            device_id={"tp": target},
            device_id_type=MESH,
        )

    def rim_copy(target):
        return pltpu.make_async_remote_copy(
            src_ref=hidden.at[pl.ds(rows - RIM, RIM)],
            dst_ref=rim,
            send_sem=rim_send.at[target],
            recv_sem=rim_recv,
            device_id={"seq": seq + 1, "tp": target},
            device_id_type=MESH,
        )

    @pl.when(jnp.logical_and(seq < last_seq, me == last_tp))
    def _():
        for target in range(n_tp):
            rim_copy(target).start()

    if square:

        @pl.when(me == 1)
        def _():
            for target in (2, 3):
                middle_copy(target).start()

        for step, half in ((1, 1), (2, 0), (1, 0), (2, 1)):
            part_copy(step, half).start()
    else:
        for step in range(1, n_tp):
            token_copy(step).start()

    @pl.when(seq == 0)
    def _():
        rim[...] = jnp.zeros_like(rim)
        st_in[...] = jnp.zeros_like(st_in)

    for load in loads + smalls:
        load.wait()

    def project(block, at):
        def one(b, carry):
            full = jnp.dot(block, weights[b], preferred_element_type=jnp.float32)
            rounded = full.astype(jnp.bfloat16).astype(jnp.float32)
            proj[b, pl.ds(pl.multiple_of(at, 16), block.shape[0]), :] = jnp.where(b < 3, rounded, full)
            return carry

        lax.fori_loop(0, 4, one, 0)

    def project_slot(slot):
        at = pl.multiple_of(slot * rows, 16)
        project(tokens[pl.ds(at, rows), :], RIM + at)

    def project_rim():
        @pl.when(seq > 0)
        def _():
            pltpu.make_async_copy(hidden.at[pl.ds(0, RIM)], rim, rim_recv).wait()

        project(rim[...], 0)

    down = lax.broadcasted_iota(jnp.int32, (CHUNK, CHUNK), 0)
    across = lax.broadcasted_iota(jnp.int32, (CHUNK, CHUNK), 1)
    eye = (down == across).astype(jnp.float32)
    wide = lax.broadcasted_iota(jnp.int32, (head_dim, 2 * head_dim), 0) + head_dim
    start = (wide == lax.broadcasted_iota(jnp.int32, (head_dim, 2 * head_dim), 1)).astype(jnp.float32)
    for h in range(heads):
        state[h] = start

    wdb = low(jnp.concatenate([wdb_ref[0].astype(jnp.float32), wdb_ref[1].astype(jnp.float32)], axis=0))

    def prepare(c):
        r0 = pl.multiple_of(c * CHUNK, CHUNK)
        scalars = lax.dot_general(
            wdb, tokens[pl.ds(r0, CHUNK), :], NT, preferred_element_type=jnp.float32
        )
        per_head = []
        for h in range(heads):
            cols = slice(h * head_dim, (h + 1) * head_dim)
            branch = []
            for b in range(3):
                window = proj[b, pl.ds(r0 + 8, CHUNK + 8), cols]
                conv = jnp.zeros((CHUNK, head_dim), jnp.float32)
                for i in range(taps):
                    offset = 9 - taps + i
                    tap = conv_ref[b, i : i + 1, cols].astype(jnp.float32)
                    conv = conv + window[offset : offset + CHUNK] * tap
                branch.append(silu(conv).astype(jnp.bfloat16).astype(jnp.float32))
            q = unit_rows(branch[0]) * (1.0 / math.sqrt(head_dim))
            k = unit_rows(branch[1])
            v = branch[2]
            u = scalars[h : h + 1, :] + bias_ref[0:1, h : h + 1]
            log_row = -rate_ref[0:1, h : h + 1] * (jnp.maximum(u, 0.0) + jnp.log1p(jnp.exp(-jnp.abs(u))))
            rate_row = 1.0 / (1.0 + jnp.exp(-scalars[heads + h : heads + h + 1, :]))
            cum_col = jnp.sum(jnp.where(across <= down, log_row, 0.0), axis=1, keepdims=True)
            cum_row = jnp.sum(jnp.where(across == down, cum_col, 0.0), axis=0, keepdims=True)
            rate_col = jnp.sum(jnp.where(across == down, rate_row, 0.0), axis=1, keepdims=True)
            end = cum_col[CHUNK - 1 : CHUNK, :]
            gap = jnp.exp(jnp.where(across <= down, cum_col - cum_row, 0.0))
            weight = jnp.where(across <= down, gap, 0.0) * rate_row
            mixing = jnp.where(across < down, weight * dot(k, k, NT), 0.0)
            attend = weight * dot(q, k, NT)
            run = jnp.exp(cum_col)
            tail = rate_col * jnp.exp(end - cum_col)
            q_runs[c, h] = low(q * run)
            k_tails[c, h] = low(k * tail)
            attends[c, h] = low(attend)
            fades[c, h] = jnp.broadcast_to(jnp.exp(end), (1, head_dim))
            per_head.append((mixing, low(jnp.concatenate([v, k * run], axis=1))))
        return per_head

    def local(chunks):
        chains = [(c, h) + item for c in chunks for h, item in enumerate(prepare(c))]
        inverse = [None] * len(chains)
        size = 1
        while size < CHUNK:
            half = (down // size) % 2 == 1
            lower = jnp.logical_and(half, across // size == down // size - 1)
            for i, (_, _, mixing, _) in enumerate(chains):
                corner = jnp.where(lower, mixing, 0.0)
                if size == 1:
                    inverse[i] = eye - corner
                else:
                    inverse[i] = inverse[i] - dot(dot(inverse[i], corner), inverse[i])
            size *= 2
        for i, (c, h, _, right) in enumerate(chains):
            solves[c, h] = dot(inverse[i], right)

    def advance(c, carry):
        r0 = pl.multiple_of(c * CHUNK, CHUNK)
        for h in range(heads):
            solved = solves[c, h]
            held = state[h]
            fresh = solved[:, :head_dim]
            fresh = jnp.concatenate([fresh, jnp.zeros_like(fresh)], axis=1)
            fresh = fresh - dot(solved[:, head_dim:], held)
            read = dot(q_runs[c, h], held) + dot(attends[c, h], fresh)
            fade = jnp.concatenate([fades[c, h]] * 2, axis=1)
            state[h] = fade * held + dot(k_tails[c, h], fresh, TN)
            outs[h, pl.ds(r0, CHUNK), :] = read[:, :head_dim]
            deltas[h, pl.ds(r0, CHUNK), :] = low(read[:, head_dim:])
        return carry

    count = total // CHUNK
    own.wait()
    project_slot(me)
    if square:
        part_copy(1, 1).wait_recv()
        relay_copy(1).start()
        part_copy(2, 0).wait_recv()
        relay_copy(0).start()
        project_rim()

        @pl.when(me >= 2)
        def _():
            pltpu.make_async_copy(hidden.at[pl.ds(0, RIM)], middle, mid_recv).wait()
            project(middle[...], 2 * rows)

        part_copy(1, 0).wait_recv()
        project_slot(peer_of(me, 1, n_tp))
        first = 2 * (me // 2)
        local((first, first + 1))
        part_copy(2, 1).wait_recv()
        project_slot(peer_of(me, 2, n_tp))
        relay_copy(0).wait_recv()
        relay_copy(1).wait_recv()
        project_slot(peer_of(me, 3, n_tp))
        local((2 - first, 3 - first))
    else:
        for step in range(1, n_tp):
            token_copy(step).wait_recv()
            if n_tp & (n_tp - 1):
                project_slot(lax.rem(me - step + n_tp, n_tp))
            else:
                project_slot(peer_of(me, step, n_tp))
        project_rim()
        lax.fori_loop(0, count, lambda c, carry: (local((c,)), carry)[1], 0)
    lax.fori_loop(0, count, advance, 0, unroll=True)

    def state_copy(h):
        return pltpu.make_async_remote_copy(
            src_ref=st_out.at[h],
            dst_ref=st_in.at[h],
            send_sem=st_send.at[h],
            recv_sem=st_recv.at[h],
            device_id={"seq": seq + 1},
            device_id_type=MESH,
        )

    for h in range(heads):

        @pl.when(seq > 0)
        def _():
            pltpu.make_async_copy(st_out.at[h], st_in.at[h], st_recv.at[h]).wait()

        @pl.when(seq < last_seq)
        def _():
            mine = state[h]
            st_out[h] = low(mine[:, :head_dim] + dot(mine[:, head_dim:], st_in[h]))
            state_copy(h).start()

    for h in range(heads):
        cols = slice(h * head_dim, (h + 1) * head_dim)
        read = outs[h] + dot(deltas[h], st_in[h])
        scale = lax.rsqrt(jnp.mean(read * read, axis=-1, keepdims=True) + 1e-06)
        gate = silu(proj[3, pl.ds(RIM, total), cols])
        out_ref[:, cols] = low(read * scale * gain_ref[...] * gate)

    if square:
        for half in range(2):
            part_copy(1, half).wait_send()
            part_copy(2, half).wait_send()
            relay_copy(half).wait_send()

        @pl.when(me == 1)
        def _():
            for target in (2, 3):
                middle_copy(target).wait_send()
    else:
        for step in range(1, n_tp):
            token_copy(step).wait_send()

    @pl.when(jnp.logical_and(seq < last_seq, me == last_tp))
    def _():
        for target in range(n_tp):
            rim_copy(target).wait_send()

    @pl.when(seq < last_seq)
    def _():
        for h in range(heads):
            state_copy(h).wait_send()


def plain_device(
    n_seq, n_tp, hidden, w_qkv, w_gate, w_decay_beta, conv_weight, decay_rate, dt_bias, norm_gain
):
    width = hidden.shape[1]
    heads = decay_rate.shape[0]
    head_dim = norm_gain.shape[0]
    columns = heads * head_dim
    rows = hidden.shape[0]
    total = rows * n_tp
    vmem, anywhere = pl.BlockSpec(memory_space=pltpu.VMEM), pl.BlockSpec(memory_space=pl.ANY)
    dma = pltpu.SemaphoreType.DMA
    count = total // CHUNK
    return pl.pallas_call(
        functools.partial(kernel, n_seq, n_tp),
        out_shape=jax.ShapeDtypeStruct((total, columns), jnp.bfloat16),
        in_specs=[anywhere] * 8,
        out_specs=vmem,
        scratch_shapes=[
            pltpu.VMEM((1, heads), jnp.float32),
            pltpu.VMEM((1, heads), jnp.float32),
            pltpu.VMEM((2, heads, width), jnp.bfloat16),
            pltpu.VMEM((3, conv_weight.shape[0], columns), jnp.bfloat16),
            pltpu.VMEM((1, head_dim), jnp.float32),
            dma((5,)),
            pltpu.VMEM((total, width), jnp.bfloat16),
            pltpu.VMEM((RIM, width), jnp.bfloat16),
            pltpu.VMEM((4, width, columns), jnp.bfloat16),
            pltpu.VMEM((4, RIM + total, columns), jnp.float32),
            pltpu.VMEM((heads, head_dim, 2 * head_dim), jnp.float32),
            pltpu.VMEM((heads, total, head_dim), jnp.float32),
            pltpu.VMEM((heads, total, head_dim), jnp.bfloat16),
            pltpu.VMEM((heads, head_dim, head_dim), jnp.bfloat16),
            pltpu.VMEM((heads, head_dim, head_dim), jnp.bfloat16),
            dma((n_tp, 2)),
            dma((n_tp, 2)),
            dma((4,)),
            dma((n_tp,)),
            dma,
            dma((heads,)),
            dma((heads,)),
            pltpu.VMEM((RIM, width), jnp.bfloat16),
            dma((2,)),
            dma,
            pltpu.VMEM((count, heads, CHUNK, 2 * head_dim), jnp.float32),
            pltpu.VMEM((count, heads, CHUNK, head_dim), jnp.bfloat16),
            pltpu.VMEM((count, heads, CHUNK, head_dim), jnp.bfloat16),
            pltpu.VMEM((count, heads, CHUNK, CHUNK), jnp.bfloat16),
            pltpu.VMEM((count, heads, 1, head_dim), jnp.float32),
        ],
        compiler_params=pltpu.CompilerParams(
            collective_id=0, has_side_effects=True, vmem_limit_bytes=60 * 1024 * 1024
        ),
    )(
        decay_rate.reshape(1, heads), dt_bias.reshape(1, heads), hidden,
        w_qkv.transpose(1, 0, 2), w_gate, w_decay_beta.transpose(1, 2, 0),
        conv_weight.transpose(1, 0, 2), norm_gain.reshape(1, head_dim),
    )


def fast_kernel(
    n_seq, rate_hbm, bias_hbm, hidden, w_qkv, w_gate, wdb_hbm, conv_hbm, gain_hbm, out_ref,
    rate_ref, bias_ref, wdb_ref, conv_ref, gain_ref, small_sem,
    tokens, rim, weights, proj_k, proj_v, proj_q, gates, half_taps, masks,
    own_sem, tok_send, tok_recv, w_sem, rim_send, rim_recv,
    betas, keys, decays, runs, fades, solves, maps, pairs, pair_fades, qeffs, outs, deltas,
    map_out, map_in, fade_out, fade_in, joined, joined_b, joined_f, far_in, far_fade,
    map_send, map_recv, fade_send, fade_recv, far_send, far_recv, far_fade_send, far_fade_recv,
    st_in, st_out, held, st_send, st_recv, fw_send, skip_send,
):
    seq, me = lax.axis_index("seq"), lax.axis_index("tp")
    last_seq = n_seq - 1
    odd = lax.rem(seq, 2) == 1
    even = lax.rem(seq, 2) == 0
    rows = hidden.shape[0]
    total = tokens.shape[0]
    heads = rate_ref.shape[1]
    dim = gain_ref.shape[1]
    taps = conv_ref.shape[1]
    count = total // CHUNK
    half_rows = rows // 2
    proj = (proj_k, proj_v, proj_q)
    tail_at = rows - RIM

    own = pltpu.make_async_copy(hidden, tokens.at[pl.ds(me * rows, rows)], own_sem)
    own.start()
    order = (1, 2, 0)
    loads = [pltpu.make_async_copy(w_qkv.at[b], weights.at[i], w_sem.at[i]) for i, b in enumerate(order)]
    loads.append(pltpu.make_async_copy(w_gate, weights.at[3], w_sem.at[3]))
    small = [(rate_hbm, rate_ref), (bias_hbm, bias_ref), (wdb_hbm, wdb_ref), (conv_hbm, conv_ref), (gain_hbm, gain_ref)]
    smalls = [pltpu.make_async_copy(src, dst, small_sem.at[i]) for i, (src, dst) in enumerate(small)]
    for load in smalls:
        load.start()

    barrier = pltpu.get_barrier_semaphore()

    def greet(where):
        pl.semaphore_signal(barrier, inc=1, device_id=where, device_id_type=MESH)

    peers = [peer_of(me, step, 4) for step in range(4)]
    for step in range(1, 3):
        greet({"tp": peers[step]})

    @pl.when(seq > 0)
    def _():
        greet({"seq": seq - 1})

    @pl.when(seq < last_seq)
    def _():
        greet({"seq": seq + 1})

    @pl.when(jnp.logical_and(odd, seq > 1))
    def _():
        greet({"seq": seq - 2})

    @pl.when(jnp.logical_and(odd, seq < last_seq))
    def _():
        greet({"seq": seq + 2})

    @pl.when(seq == last_seq)
    def _():
        greet({"seq": last_seq - 4})

    @pl.when(seq == last_seq - 4)
    def _():
        greet({"seq": last_seq})

    is_odd = lax.rem(seq, 2)
    before = (seq + last_seq) // n_seq
    after = (2 * last_seq - seq) // n_seq
    before2 = (seq + n_seq - 2) // n_seq
    skips = seq // last_seq + ((seq + 1) // (last_seq - 3)) * ((last_seq - 3) // (seq + 1))
    pl.semaphore_wait(barrier, 2 + before + after + is_odd * (before2 + after) + skips)

    quarter = half_rows // 2
    pieces = ((0, quarter), (quarter, quarter), (half_rows, tail_at - half_rows), (tail_at, RIM))

    def piece_copy(step, piece):
        at, size = pieces[piece]
        where = tokens.at[pl.ds(me * rows + at, size)]
        return pltpu.make_async_remote_copy(
            src_ref=where,
            dst_ref=where,
            send_sem=tok_send.at[step, piece],
            recv_sem=tok_recv.at[step, piece],
            device_id={"tp": peers[step]},
            device_id_type=MESH,
        )

    def relay_copy(piece):
        at, size = pieces[piece]
        via = 1 if piece < 2 else 2
        there = tokens.at[pl.ds(peers[3 - via] * rows + at, size)]
        return pltpu.make_async_remote_copy(
            src_ref=there,
            dst_ref=there,
            send_sem=tok_send.at[3, piece],
            recv_sem=tok_recv.at[3, piece],
            device_id={"tp": peers[via]},
            device_id_type=MESH,
        )

    def rim_copy():
        return pltpu.make_async_remote_copy(
            src_ref=tokens.at[pl.ds(total - RIM, RIM)],
            dst_ref=rim,
            send_sem=rim_send,
            recv_sem=rim_recv,
            device_id={"seq": seq + 1},
            device_id_type=MESH,
        )

    own.wait()
    for step, piece in ((1, 3), (2, 3), (1, 2), (2, 0)):
        piece_copy(step, piece).start()
    for load in loads:
        load.start()

    @pl.when(seq == 0)
    def _():
        rim[...] = jnp.zeros_like(rim)

    down = lax.broadcasted_iota(jnp.int32, (CHUNK, CHUNK), 0)
    across = lax.broadcasted_iota(jnp.int32, (CHUNK, CHUNK), 1)
    eye = low((down == across).astype(jnp.float32))
    edges = (1, 2, 8, 32, CHUNK)
    for i in range(4):
        inside = down // edges[i + 1] == across // edges[i + 1]
        apart = down // edges[i] != across // edges[i]
        masks[i] = low(jnp.where(jnp.logical_and(inside, apart), 1.0, 0.0))

    for load in smalls:
        load.wait()
    for b in range(3):
        for i in range(taps):
            row = conv_ref[b, i : i + 1, :].astype(jnp.float32) * 0.5
            for h in range(heads):
                cols = slice(h * dim, (h + 1) * dim)
                half_taps[b, i, h] = jnp.broadcast_to(row[:, cols], (8, dim))
    wdb = low(jnp.concatenate([wdb_ref[0].astype(jnp.float32), wdb_ref[1].astype(jnp.float32)], axis=0))

    def project(block, branches, places):
        for b in branches:
            full = jnp.dot(block, weights[b], preferred_element_type=jnp.float32)
            if b < 3:
                full = full.astype(jnp.bfloat16).astype(jnp.float32)
            for start, size, at, edge in places:
                for h in range(heads):
                    got = full[start : start + size, h * dim : (h + 1) * dim]
                    if b < 3:
                        proj[b][h, pl.ds(pl.multiple_of(at + RIM, RIM), size), :] = got
                    elif not edge:
                        gates[h, pl.ds(pl.multiple_of(at, RIM), size), :] = got

    def take(runs_of_rows):
        blocks, places, start = [], [], 0
        for slot, at, size in runs_of_rows:
            begin = pl.multiple_of(slot * rows + at, RIM)
            blocks.append(tokens[pl.ds(begin, size), :])
            places.append((start, size, begin, size == RIM))
            start += size
        return jnp.concatenate(blocks, axis=0), places

    def half_silu(half):
        return half + half * jnp.tanh(half)

    def branch(b, h, r0):
        conv = None
        for i in range(taps):
            window = proj[b][h, pl.ds(r0 + (RIM + 1 - taps + i), CHUNK), :]
            term = window.reshape(CHUNK // 8, 8, dim) * half_taps[order[b], i, h][None]
            conv = term if conv is None else conv + term
        return half_silu(conv).astype(jnp.bfloat16).reshape(CHUNK, dim)

    def gate_rows(c):
        r0 = pl.multiple_of(c * CHUNK, CHUNK)
        scalars = lax.dot_general(
            wdb, tokens[pl.ds(r0, CHUNK), :], NT, preferred_element_type=jnp.float32
        )
        for h in range(heads):
            u = scalars[h : h + 1, :] + bias_ref[0:1, h : h + 1]
            log_row = -rate_ref[0:1, h : h + 1] * (jnp.maximum(u, 0.0) + jnp.log1p(jnp.exp(-jnp.abs(u))))
            rate_row = 1.0 / (1.0 + jnp.exp(-scalars[heads + h : heads + h + 1, :]))
            cum_col = jnp.sum(jnp.where(across <= down, log_row, 0.0), axis=1, keepdims=True)
            cum_row = jnp.sum(jnp.where(across == down, cum_col, 0.0), axis=0, keepdims=True)
            rate_col = jnp.sum(jnp.where(across == down, rate_row, 0.0), axis=1, keepdims=True)
            end = cum_col[CHUNK - 1 : CHUNK, :]
            gap = jnp.exp(jnp.where(across <= down, cum_col - cum_row, 0.0))
            decays[c, h] = jnp.where(across <= down, gap, 0.0) * rate_row
            runs[c, h] = jnp.broadcast_to(jnp.exp(cum_col), (CHUNK, dim))
            betas[c, h] = jnp.broadcast_to(rate_col * jnp.exp(end - cum_col), (CHUNK, dim))
            fades[c, h] = jnp.broadcast_to(jnp.exp(end), (1, dim))

    def prepare(c):
        r0 = pl.multiple_of(c * CHUNK, CHUNK)
        chains = []
        for h in range(heads):
            k = unit_rows(branch(0, h, r0).astype(jnp.float32))
            low_k = low(k)
            keys[c, h] = low_k
            mixing = low(jnp.where(across < down, decays[c, h] * dot(low_k, low_k, NT), 0.0))
            chains.append((c, h, mixing, low(k * runs[c, h]), low(k * betas[c, h])))
        return chains

    def project_values(block, at, part):
        size = heads * dim // 2
        full = jnp.dot(block, weights[1, :, pl.ds(part * size, size)], preferred_element_type=jnp.float32)
        full = full.astype(jnp.bfloat16).astype(jnp.float32)
        for i in range(heads // 2):
            got = full[:, i * dim : (i + 1) * dim]
            proj_v[part * (heads // 2) + i, pl.ds(pl.multiple_of(at + RIM, RIM), rows), :] = got

    def solve(chains, values=None):
        inverse = [eye - mixing * masks[0] for _, _, mixing, _, _ in chains]
        for level in (1, 2):
            step = [low(dot(d, item[2] * masks[level])) for d, item in zip(inverse, chains)]
            if values and level == 1:
                project_values(*values, 0)
            both = [dot(x, jnp.concatenate([low(d), x], axis=1)) for x, d in zip(step, inverse)]
            if values and level == 1:
                project_values(*values, 1)
            first = [d.astype(jnp.float32) - p[:, :CHUNK] for p, d in zip(both, inverse)]
            inverse = [q + dot(p[:, CHUNK:], q) for p, q in zip(both, first)]
        both = [
            dot(d, jnp.concatenate([mixing * masks[3], branch(1, h, pl.multiple_of(c * CHUNK, CHUNK)), k_run], axis=1))
            for d, (c, h, mixing, k_run, _) in zip(inverse, chains)
        ]
        again = [dot(p[:, :CHUNK], p) for p in both]
        first = [p[:, CHUNK:] - a[:, CHUNK:] for p, a in zip(both, again)]
        solved = [low(q + dot(a[:, :CHUNK], q)) for a, q in zip(again, first)]
        for item, value in zip(chains, solved):
            c, h = item[:2]
            solves[c, h] = value
            got = dot(item[4], value, TN)
            maps[c, h] = jnp.concatenate([got[:, :dim], -got[:, dim:]], axis=1)

    def queries(c):
        r0 = pl.multiple_of(c * CHUNK, CHUNK)
        for h in range(heads):
            q = unit_rows(branch(2, h, r0).astype(jnp.float32)) * (1.0 / math.sqrt(dim))
            attend = decays[c, h] * dot(q, keys[c, h], NT)
            got = dot(attend, solves[c, h])
            outs[h, pl.ds(r0, CHUNK), :] = got[:, :dim]
            qeffs[h, pl.ds(r0, CHUNK), :] = q * runs[c, h] - got[:, dim:]

    def join(late, early):
        (high, keep), (whole, fade) = late, early
        got = dot(high[:, dim:], whole)
        left = keep * whole[:, :dim] + high[:, :dim] + got[:, :dim]
        right = keep * whole[:, dim:] + fade * high[:, dim:] + got[:, dim:]
        return jnp.concatenate([left, right], axis=1), keep * fade

    def pair_up(p):
        for h in range(heads):
            whole, fade = join((maps[2 * p + 1, h], fades[2 * p + 1, h]), (maps[2 * p, h], fades[2 * p, h]))
            pairs[p, h] = whole
            pair_fades[p, h] = fade

    piece_copy(1, 3).wait_recv()
    relay_copy(3).start()
    for step, piece in ((1, 0), (1, 1), (2, 1), (2, 2)):
        piece_copy(step, piece).start()

    for load in loads:
        load.wait()
    block, places = take(((me, 0, rows),))
    project(block, range(4), places)

    piece_copy(2, 3).wait_recv()
    relay_copy(3).wait_recv()

    @pl.when(seq < last_seq)
    def _():
        rim_copy().start()

    piece_copy(1, 2).wait_recv()
    relay_copy(2).start()
    piece_copy(2, 0).wait_recv()
    relay_copy(0).start()

    @pl.when(seq > 0)
    def _():
        pltpu.make_async_copy(tokens.at[pl.ds(0, RIM)], rim, rim_recv).wait()

    block, places = take(((peers[1], half_rows, half_rows), (peers[2], 0, quarter), (peers[3], tail_at, RIM)))
    block = jnp.concatenate([block, rim[...]], axis=0)
    project(block, range(4), places + [(rows - RIM, RIM, -RIM, True)])
    piece_copy(2, 1).wait_recv()
    relay_copy(1).start()
    gate_rows(me)
    solve(prepare(me))
    queries(me)

    piece_copy(1, 0).wait_recv()
    piece_copy(1, 1).wait_recv()
    piece_copy(2, 2).wait_recv()
    late, late_places = take(((peers[1], 0, half_rows), (peers[2], quarter, rows - quarter)))
    gate_rows(peers[1])
    gate_rows(peers[2])
    project(late, range(2), late_places)
    solve(prepare(peers[1]) + prepare(peers[2]))
    pair_up(me // 2)

    for piece in range(3):
        relay_copy(piece).wait_recv()
    block, places = take(((peers[3], 0, rows),))
    project(block, range(1), places)
    gate_rows(peers[3])
    solve(prepare(peers[3]), (block, places[0][2]))
    for h in range(heads):
        fade_out[h] = fades[0, h] * fades[1, h] * (fades[2, h] * fades[3, h])
    pair_up(1 - me // 2)
    for h in range(heads):
        whole, fade = join((pairs[1, h], pair_fades[1, h]), (pairs[0, h], pair_fades[0, h]))
        joined_b[h] = whole[:, :dim]
        joined[h] = whole[:, dim:]
        joined_f[h] = fade
        map_out[h] = low(whole)

    def map_copy(h):
        return pltpu.make_async_remote_copy(
            src_ref=map_out.at[h], dst_ref=map_in.at[h], send_sem=map_send.at[h], recv_sem=map_recv.at[h],
            device_id={"seq": seq + 1}, device_id_type=MESH,
        )

    def fade_copy():
        return pltpu.make_async_remote_copy(
            src_ref=fade_out, dst_ref=fade_in, send_sem=fade_send, recv_sem=fade_recv,
            device_id={"seq": seq + 1}, device_id_type=MESH,
        )

    def state_copy(h):
        return pltpu.make_async_remote_copy(
            src_ref=st_out.at[h], dst_ref=st_in.at[h], send_sem=st_send.at[h], recv_sem=st_recv.at[h],
            device_id={"seq": seq + 2}, device_id_type=MESH,
        )

    def skip_copy(h):
        return pltpu.make_async_remote_copy(
            src_ref=st_out.at[h], dst_ref=st_in.at[h], send_sem=skip_send.at[h], recv_sem=st_recv.at[h],
            device_id={"seq": seq + 4}, device_id_type=MESH,
        )

    def far_copy(h):
        return pltpu.make_async_remote_copy(
            src_ref=map_out.at[h], dst_ref=far_in.at[h], send_sem=far_send.at[h], recv_sem=far_recv.at[h],
            device_id={"seq": seq + 2}, device_id_type=MESH,
        )

    def far_fade_copy():
        return pltpu.make_async_remote_copy(
            src_ref=joined_f, dst_ref=far_fade, send_sem=far_fade_send, recv_sem=far_fade_recv,
            device_id={"seq": seq + 2}, device_id_type=MESH,
        )

    def share_copy(h, source):
        return pltpu.make_async_remote_copy(
            src_ref=source.at[h], dst_ref=st_in.at[h], send_sem=fw_send.at[h], recv_sem=st_recv.at[h],
            device_id={"seq": seq - 1}, device_id_type=MESH,
        )

    @pl.when(even)
    def _():
        fade_copy().start()
        for h in range(heads):
            map_copy(h).start()

    @pl.when(seq == 0)
    def _():
        for h in range(heads):
            held[h] = jnp.zeros((dim, dim), jnp.bfloat16)

    def send_on(skip):
        def send(h):
            if skip:
                skip_copy(h).start()
            else:
                state_copy(h).start()

        return send

    def sent_map(h):
        return map_in[h].astype(jnp.float32), fade_in[h]

    def begin(skip):
        for h in range(heads):
            map_copy(h).wait_recv()
            state = map_in[h, :, :dim]
            base = joined_f[h] * state.astype(jnp.float32) + joined_b[h]
            st_out[h] = low(base + dot(joined[h], state))
            send_on(skip)(h)
        fade_copy().wait_recv()
        for h in range(heads):
            held[h] = map_in[h, :, :dim]
            if skip:
                state_copy(h).start()

    def compose(ends):
        fade_copy().wait_recv()
        for h in range(heads):
            map_copy(h).wait_recv()
        mine = [(jnp.concatenate([joined_b[h], joined[h]], axis=1), joined_f[h]) for h in range(heads)]
        both = [join(mine[h], sent_map(h)) for h in range(heads)]
        for h, (whole, fade) in enumerate(both):
            joined_b[h] = whole[:, :dim]
            joined[h] = whole[:, dim:]
            joined_f[h] = fade
            map_out[h] = low(whole)

        if ends:
            far_fade_copy().start()
            for h in range(heads):
                far_copy(h).start()

    @pl.when(seq == 1)
    def _():
        begin(last_seq == 5)

    def carry(h, state, whole, fade):
        wide = state.astype(jnp.float32)
        return low(fade * wide + whole[:, :dim].astype(jnp.float32) + dot(whole[:, dim:], state))

    def pass_on(more, skip):
        for h in range(heads):
            state_copy(h).wait_recv()
            if more:
                state = st_in[h]
                wide = joined_f[h] * state.astype(jnp.float32) + joined_b[h]
                st_out[h] = low(wide + dot(joined[h], state))
                send_on(skip)(h)
            share_copy(h, st_in).start()
        for h in range(heads):
            if more and skip:
                state_copy(h).start()
            held[h] = carry(h, st_in[h], map_in[h], fade_in[h])

    def end_chain():
        fade_copy().wait_recv()
        for h in range(heads):
            map_copy(h).wait_recv()
        far_fade_copy().wait_recv()
        for h in range(heads):
            far_copy(h).wait_recv()
            state_copy(h).wait_recv()
            st_out[h] = carry(h, st_in[h], far_in[h], far_fade[h])
            share_copy(h, st_out).start()
        for h in range(heads):
            held[h] = carry(h, st_out[h], map_in[h], fade_in[h])

    @pl.when(seq == last_seq - 2)
    def _():
        compose(True)

    project(late, range(2, 4), late_places)

    @pl.when(jnp.logical_and(jnp.logical_and(odd, seq > 1), seq < last_seq - 2))
    def _():
        compose(False)


    queries(peers[1])

    @pl.when(jnp.logical_and(jnp.logical_and(odd, seq > 1), seq < last_seq - 4))
    def _():
        pass_on(True, False)

    if last_seq > 5:

        @pl.when(seq == last_seq - 4)
        def _():
            pass_on(True, True)

    queries(peers[2])


    project(block, range(2, 4), places)
    queries(peers[3])
    for h in range(heads):
        gates[h] = half_silu(0.5 * gates[h]) * gain_ref[...]
        third, fade = join((maps[2, h], fades[2, h]), (pairs[0, h], pair_fades[0, h]))
        for c in range(count):
            at = pl.ds(c * CHUNK, CHUNK)
            qeff = qeffs[h, at, :]
            if c == 0:
                deltas[h, at, :] = low(qeff)
            else:
                prefix, keep = (
                    (maps[0, h], fades[0, h]), (pairs[0, h], pair_fades[0, h]), (third, fade)
                )[c - 1]
                got = dot(qeff, prefix)
                outs[h, at, :] = outs[h, at, :] + got[:, :dim]
                deltas[h, at, :] = low(keep * qeff + got[:, dim:])

    @pl.when(seq == last_seq - 2)
    def _():
        pass_on(False, False)

    @pl.when(seq == last_seq)
    def _():
        end_chain()

    for h in range(heads):

        @pl.when(jnp.logical_and(even, seq > 0))
        def _():
            state_copy(h).wait_recv()
            held[h] = st_in[h]

        cols = slice(h * dim, (h + 1) * dim)
        read = outs[h] + dot(deltas[h], held[h])
        scale = lax.rsqrt(jnp.mean(read * read, axis=-1, keepdims=True) + 1e-06)
        out_ref[:, cols] = low(read * scale * gates[h])

    for step in range(1, 4):
        for piece in range(4):
            if step == 3:
                relay_copy(piece).wait_send()
            else:
                piece_copy(step, piece).wait_send()

    @pl.when(seq < last_seq)
    def _():
        rim_copy().wait_send()

    @pl.when(even)
    def _():
        fade_copy().wait_send()
        for h in range(heads):
            map_copy(h).wait_send()

    @pl.when(jnp.logical_and(odd, seq > 1))
    def _():
        for h in range(heads):
            share_copy(h, st_in).wait_send()

    @pl.when(jnp.logical_and(odd, seq <= last_seq - 4))
    def _():
        for h in range(heads):
            state_copy(h).wait_send()

    @pl.when(seq == last_seq - 4)
    def _():
        for h in range(heads):
            skip_copy(h).wait_send()

    @pl.when(seq == last_seq - 2)
    def _():
        far_fade_copy().wait_send()
        for h in range(heads):
            far_copy(h).wait_send()


def fast_device(n_seq, hidden, w_qkv, w_gate, w_decay_beta, conv_weight, decay_rate, dt_bias, norm_gain):
    rows, width = hidden.shape
    heads = decay_rate.shape[0]
    dim = norm_gain.shape[0]
    taps = conv_weight.shape[0]
    columns = heads * dim
    total = rows * 4
    count = total // CHUNK
    dma = pltpu.SemaphoreType.DMA
    f32, bf16 = jnp.float32, jnp.bfloat16
    operands = (
        decay_rate.reshape(1, heads), dt_bias.reshape(1, heads), hidden,
        w_qkv.transpose(1, 0, 2), w_gate, w_decay_beta.transpose(1, 2, 0),
        conv_weight.transpose(1, 0, 2), norm_gain.reshape(1, dim),
    )
    return pl.pallas_call(
        functools.partial(fast_kernel, n_seq),
        out_shape=jax.ShapeDtypeStruct((total, columns), bf16),
        in_specs=[pl.BlockSpec(memory_space=pl.ANY)] * 8,
        out_specs=pl.BlockSpec(memory_space=pltpu.VMEM),
        scratch_shapes=[
            pltpu.VMEM((1, heads), f32),
            pltpu.VMEM((1, heads), f32),
            pltpu.VMEM((2, heads, width), bf16),
            pltpu.VMEM((3, taps, columns), bf16),
            pltpu.VMEM((1, dim), f32),
            dma((5,)),
            pltpu.VMEM((total, width), bf16),
            pltpu.VMEM((RIM, width), bf16),
            pltpu.VMEM((4, width, columns), bf16),
            pltpu.VMEM((heads, RIM + total, dim), f32),
            pltpu.VMEM((heads, RIM + total, dim), f32),
            pltpu.VMEM((heads, RIM + total, dim), f32),
            pltpu.VMEM((heads, total, dim), f32),
            pltpu.VMEM((3, taps, heads, 8, dim), f32),
            pltpu.VMEM((4, CHUNK, CHUNK), bf16),
            dma,
            dma((4, 4)),
            dma((4, 4)),
            dma((4,)),
            dma,
            dma,
            pltpu.VMEM((count, heads, CHUNK, dim), f32),
            pltpu.VMEM((count, heads, CHUNK, dim), bf16),
            pltpu.VMEM((count, heads, CHUNK, CHUNK), f32),
            pltpu.VMEM((count, heads, CHUNK, dim), f32),
            pltpu.VMEM((count, heads, 1, dim), f32),
            pltpu.VMEM((count, heads, CHUNK, 2 * dim), bf16),
            pltpu.VMEM((count, heads, dim, 2 * dim), f32),
            pltpu.VMEM((2, heads, dim, 2 * dim), f32),
            pltpu.VMEM((2, heads, 1, dim), f32),
            pltpu.VMEM((heads, total, dim), f32),
            pltpu.VMEM((heads, total, dim), f32),
            pltpu.VMEM((heads, total, dim), bf16),
            pltpu.VMEM((heads, dim, 2 * dim), bf16),
            pltpu.VMEM((heads, dim, 2 * dim), bf16),
            pltpu.VMEM((heads, 1, dim), f32),
            pltpu.VMEM((heads, 1, dim), f32),
            pltpu.VMEM((heads, dim, dim), f32),
            pltpu.VMEM((heads, dim, dim), f32),
            pltpu.VMEM((heads, 1, dim), f32),
            pltpu.VMEM((heads, dim, 2 * dim), bf16),
            pltpu.VMEM((heads, 1, dim), f32),
            dma((heads,)),
            dma((heads,)),
            dma,
            dma,
            dma((heads,)),
            dma((heads,)),
            dma,
            dma,
            pltpu.VMEM((heads, dim, dim), bf16),
            pltpu.VMEM((heads, dim, dim), bf16),
            pltpu.VMEM((heads, dim, dim), bf16),
            dma((heads,)),
            dma((heads,)),
            dma((heads,)),
            dma((heads,)),
        ],
        compiler_params=pltpu.CompilerParams(
            collective_id=0, has_side_effects=True, vmem_limit_bytes=48 * 1024 * 1024
        ),
    )(*[pltpu.with_memory_space_constraint(x, pltpu.HBM) for x in operands])


def per_device(n_seq, n_tp, hidden, *rest):
    if n_tp == 4 and hidden.shape[0] == CHUNK and n_seq % 2 == 0 and n_seq >= 6:
        return fast_device(n_seq, hidden, *rest)
    return plain_device(n_seq, n_tp, hidden, *rest)


def solution(mesh):
    return jax.shard_map(
        functools.partial(per_device, mesh.shape["seq"], mesh.shape["tp"]),
        mesh=mesh,
        in_specs=(
            P(("seq", "tp"), None),
            P(None, None, "tp"),
            P(None, "tp"),
            P(None, None, "tp"),
            P(None, None, "tp"),
            P("tp"),
            P("tp"),
            P(),
        ),
        out_specs=P("seq", "tp"),
        check_vma=False,
    )
```
